32 devices in a mesh: trait: 2 (over x), ppl: 16 (over z, y, core).
Axes of the slice: x: 2, y: 2, z: 4, core: 2. Of those that a mesh axis runs over, the one named last changes fastest.
Arguments:
- genotypes: bfloat16 [8192, 4096], P(('trait', 'ppl')), parts along dimension 0
- residual: float32 [64, 4096], P('trait', 'ppl'), parts along dimension 0, may hold values from -36 to 36
- noise_people: float32 [64, 4096], P('trait', 'ppl'), parts along dimension 0, may hold values from -6 to 6
- noise_coef: float32 [64, 4096], P('trait'), parts along dimension 0, may hold values from -6 to 6
- coef_all: float32 [64, 8192], P('trait'), parts along dimension 0, may hold values from -0.06 to 0.06
- block_index: int32 [2], P('trait'), parts along dimension 0, may hold values from 0 to 1
- prior_prec: float32 [64], P('trait'), parts along dimension 0, may hold values from 21 to 103
- sigma2_old: float32 [64], P('trait'), parts along dimension 0, may hold values from 0.5 to 2
- gamma_draw: float32 [64], P('trait'), parts along dimension 0, may hold values from 0.8 to 1.25
- valid_counts: int32 [32], P('trait'), parts along dimension 0, may hold values from 128 to 256, as said below
Outputs:
- coef_new: float32 [64, 8192], P('trait'), parts along dimension 0
- residual_new: float32 [64, 4096], P('trait', 'ppl'), parts along dimension 0
- sigma2_new: float32 [64], P('trait'), parts along dimension 0
The draws below stay inside these ranges and needn't reach their ends.
There are 2 independent parts, one for each index of `trait`. The reference program is written for one: setup_inputs(seed, part) draws one part's arguments, and reference() takes and returns one part's arrays. A program takes and returns all parts, laid end to end along the dimension named above; each array names one. Nothing has to cross between parts.
Inputs may be any that keep to these rules, and one draw needn't show every extreme that they name: `valid_counts`: each entry counts the people present in one device's 256 slots; they fill the lowest slots, and some entry equals 256.
All inputs are finite; a program needn't handle non-finite values.
Results may differ from the reference program's by a relative error of at most 0.0049.
Values may be sent and summed in bfloat16 or wider, within the bound.
No kernel may reach another device: no remote copies, remote signals or barrier semaphores. Data moves between devices by JAX's collectives and lax.ppermute only.
A program may use at most 64 MiB of HBM per device.

```python
import math
import jax
import jax.numpy as jnp
from jax import lax

ROWS_DEV = 256
BATCH = 4096
TRAITS = 32
ITERS = 4
BLOCKS = 2
PEOPLE = 4096
VARS = 8192
N_PPL = 16


def draw_genotypes(key, part):
    inner_key = jax.random.fold_in(key, 11)
    innov = jax.random.normal(inner_key, (PEOPLE, BATCH + 2), jnp.float32)
    blended = innov[:, 1:-1] + 0.45 * (innov[:, :-2] + innov[:, 2:])
    return (blended / jnp.sqrt(1.405)).astype(jnp.bfloat16)


def draw_residual(key, part):
    inner_key = jax.random.fold_in(key, 23)
    position = jnp.arange(PEOPLE, dtype=jnp.float32) / PEOPLE
    base = jax.random.normal(inner_key, (TRAITS, PEOPLE), jnp.float32)
    scale_line = 1.0 + 2.0 * position
    return jnp.clip(base, -6.0, 6.0) * scale_line[None, :]


def draw_valid_counts(key, part):
    inner_key = jax.random.fold_in(key, 7)
    key_counts, key_full = jax.random.split(inner_key)
    drawn_counts = jax.random.randint(key_counts, (N_PPL,), ROWS_DEV // 2, ROWS_DEV + 1)
    full_shard = jax.random.randint(key_full, (), 0, N_PPL)
    filled = jnp.where(jnp.arange(N_PPL) == full_shard, ROWS_DEV, drawn_counts)
    return filled.astype(jnp.int32)


def levels(rng, dims, cuts, low, high):
    factor_of, own = 1.0, jax.random.fold_in(rng, 6)
    for dim, blocks in cuts:
        steps = jnp.exp(jax.random.uniform(jax.random.fold_in(own, dim), (blocks,), jnp.float32, low / len(cuts), high / len(cuts)))
        factor_of = factor_of * jnp.repeat(steps, dims[dim] // blocks).reshape([-1 if axis == dim else 1 for axis in range(len(dims))])
    return factor_of


def normal_values(stream_key, extent, scale, limit, shards=(), kind=jnp.bfloat16):
    loudness = levels(stream_key, extent, shards, -0.22, 0.18) if shards else 1.0
    entries = jax.random.normal(stream_key, extent, jnp.float32) * scale * loudness
    return jnp.minimum(jnp.maximum(entries, -limit), limit).astype(kind)


def setup_inputs(seed: int = 0, part: int = 0) -> dict:
    seeds = jax.random.split(jax.random.key(seed), 11)
    own_keys = jax.random.split(jax.random.fold_in(seeds[10], part), 11)
    return {
        "genotypes": draw_genotypes(jax.random.fold_in(jax.random.fold_in(seeds[10], part), 71), part),
        "residual": draw_residual(jax.random.fold_in(jax.random.fold_in(seeds[10], part), 71), part),
        "noise_people": normal_values(own_keys[2], (TRAITS, PEOPLE), 1.0, 6.0, ((1, 16),), jnp.float32),
        "noise_coef": normal_values(own_keys[3], (TRAITS, BATCH), 1.0, 6.0, (), jnp.float32),
        "coef_all": normal_values(own_keys[4], (TRAITS, VARS), 0.01, 0.06, (), jnp.float32),
        "block_index": jax.random.randint(own_keys[5], (1,), 0, BLOCKS).astype(jnp.int32),
        "prior_prec": jnp.clip(jnp.exp(jax.random.uniform(own_keys[6], (TRAITS,), jnp.float32, math.log(21.0), math.log(103.0))), 21.0, 103.0),
        "sigma2_old": jnp.clip(jnp.exp(jax.random.uniform(own_keys[7], (TRAITS,), jnp.float32, math.log(0.5), math.log(2.0))), 0.5, 2.0),
        "gamma_draw": jnp.clip(jax.random.uniform(own_keys[8], (TRAITS,), jnp.float32, 0.8, 1.25), 0.8, 1.25),
        "valid_counts": draw_valid_counts(jax.random.fold_in(jax.random.fold_in(seeds[10], part), 71), part),
    }


PRIOR_DOF = 4.0
PRIOR_SCALE = 0.5

def reference(genotypes, residual, noise_people, noise_coef, coef_all, block_index, prior_prec, sigma2_old, gamma_draw, valid_counts):
    people_total = genotypes.shape[0]
    slot_ids = jnp.arange(people_total, dtype=jnp.int32)
    shard_ids = slot_ids // ROWS_DEV
    within = slot_ids % ROWS_DEV
    person_mask = (within < valid_counts[shard_ids]).astype(jnp.float32)[None, :]
    first_col = (block_index[0] * BATCH).astype(jnp.int32)
    old_coef = lax.dynamic_slice_in_dim(coef_all, first_col, BATCH, 1)
    contract = (((1,), (1,)), ((), ()))
    fitted_old = lax.dot_general(old_coef.astype(jnp.bfloat16), genotypes, contract, preferred_element_type=jnp.float32)
    partial_res = person_mask * (residual + fitted_old)
    noise_var = sigma2_old[:, None]
    ridge = prior_prec[:, None]
    target = (person_mask * (partial_res + jnp.sqrt(noise_var) * noise_people)).astype(jnp.bfloat16)
    rhs = jnp.dot(target, genotypes, preferred_element_type=jnp.float32) / noise_var + jnp.sqrt(ridge) * noise_coef
    batch_coef = jnp.zeros_like(rhs)
    fitted = jnp.zeros_like(partial_res)
    search = rhs
    direction = rhs
    norm_now = lax.optimization_barrier(jnp.sum(search * search, axis=1))
    for number in range(ITERS):
        dir_low = direction.astype(jnp.bfloat16)
        dir_full = lax.optimization_barrier(dir_low).astype(jnp.float32)
        image = person_mask * lax.dot_general(dir_low, genotypes, contract, preferred_element_type=jnp.float32)
        image_low = image.astype(jnp.bfloat16)
        applied = jnp.dot(image_low, genotypes, preferred_element_type=jnp.float32) / noise_var + ridge * dir_full
        step_size = norm_now / lax.optimization_barrier(jnp.sum(dir_full * applied, axis=1))
        batch_coef = batch_coef + step_size[:, None] * dir_full
        fitted = fitted + step_size[:, None] * image
        search = search - step_size[:, None] * applied
        norm_next = lax.optimization_barrier(jnp.sum(search * search, axis=1))
        direction = search + (norm_next / norm_now)[:, None] * direction
        norm_now = norm_next
    residual_new = partial_res - fitted
    squares = lax.optimization_barrier(jnp.sum(residual_new * residual_new, axis=1))
    present = jnp.sum(valid_counts).astype(jnp.float32)
    sigma2_new = (squares + PRIOR_DOF * PRIOR_SCALE) / ((present + PRIOR_DOF) * gamma_draw)
    coef_new = lax.dynamic_update_slice_in_dim(coef_all, batch_coef, first_col, 1)
    return (coef_new, residual_new, sigma2_new)
```

```python
import functools

import jax
import jax.numpy as jnp
from jax import lax
from jax.sharding import PartitionSpec as P

ITERS = 4
PRIOR_DOF = 4.0
PRIOR_SCALE = 0.5
CONTRACT = (((1,), (1,)), ((), ()))
LANES = 128
F32, BF16 = jnp.float32, jnp.bfloat16


def swap(x, count, distance):
    return lax.ppermute(x, "ppl", [(i, i ^ distance) for i in range(count)])


def to_parts(value):
    first = lax.reduce_precision(value, 8, 7)
    second = lax.reduce_precision(value - first, 8, 7)
    third = value - first - second
    parts = jnp.concatenate([first, second, third], axis=1).astype(BF16)
    return jnp.pad(parts, ((0, 0), (0, LANES - 3)))


def from_parts(parts):
    wide = parts.astype(F32)
    return (wide[:, 2:3] + wide[:, 1:2]) + wide[:, 0:1]


def per_device(
    count,
    genotypes,
    residual,
    noise_people,
    noise_coef,
    coef_all,
    block_index,
    prior_prec,
    sigma2_old,
    gamma_draw,
    valid_counts,
):
    rows, width = genotypes.shape
    bits = count.bit_length() - 1
    top = bits - 2
    me = lax.axis_index("ppl")
    core, place = me & 1, me >> top
    half = width // 2
    chunk = half // 4
    chips = range(1, top)
    dot_t = functools.partial(lax.dot_general, dimension_numbers=CONTRACT, preferred_element_type=F32)
    dot = functools.partial(jnp.dot, preferred_element_type=F32)

    def columns(array, side, slot):
        return lax.dynamic_slice_in_dim(array, side * half + (place ^ slot) * chunk, chunk, 1)

    x_own = jnp.concatenate([columns(genotypes, core, t) for t in range(4)], axis=1)
    x_give = jnp.concatenate([columns(genotypes, 1 - core, t) for t in range(4)], axis=1)
    x_far = swap(x_give, count, 1)

    slots = jnp.arange(rows)
    mask_own = (slots < valid_counts[me]).astype(F32)[None, :]
    mask_far = (slots < valid_counts[me ^ 1]).astype(F32)[None, :]
    first_col = block_index[0] * width
    noise_var = sigma2_old[:, None]
    ridge = prior_prec[:, None]

    def over_people(data, extra, kind):
        if extra is not None:
            tail = to_parts(extra) if kind == BF16 else jnp.broadcast_to(extra, (extra.shape[0], LANES))
        pieces = []
        for t in range(4):
            piece = data[:, t * chunk : (t + 1) * chunk].astype(kind)
            pieces.append(piece if extra is None else jnp.concatenate([piece, tail], axis=1))
        got = [pieces[0]] + [swap(pieces[t], count, t << top) for t in (1, 2, 3)]
        body = [g[:, :chunk].astype(F32) for g in got]
        total = (body[0] + body[1]) + (body[2] + body[3])
        if extra is not None:
            tails = [from_parts(g[:, chunk:]) if kind == BF16 else g[:, chunk : chunk + 1] for g in got]
            scalar = (tails[0] + tails[1]) + (tails[2] + tails[3])
            total = jnp.concatenate([total, jnp.broadcast_to(scalar, (scalar.shape[0], LANES))], axis=1)
        for bit in chips:
            total = total + swap(total, count, 1 << bit)
        return total

    old_coef = lax.dynamic_slice_in_dim(coef_all, first_col, width, 1)
    fitted_old = dot_t(old_coef.astype(BF16), genotypes)
    partial_res = mask_own * (residual + fitted_old)
    target = (mask_own * (partial_res + jnp.sqrt(noise_var) * noise_people)).astype(BF16)
    target_far = swap(target, count, 1)
    data = over_people(dot(target, x_own) + dot(target_far, x_far), None, F32)
    search = data / noise_var + jnp.sqrt(ridge) * columns(noise_coef, core, 0)

    image_own = image_far = jnp.zeros_like(partial_res)
    fitted = jnp.zeros_like(partial_res)
    direction = jnp.zeros((search.shape[0], half), F32)
    batch_half = direction
    norm_now = length = None
    for number in range(ITERS):
        low = search.astype(BF16)
        packed = jnp.concatenate([low, to_parts(jnp.sum(search * search, axis=1, keepdims=True))], axis=1)
        got = [packed] + [swap(packed, count, t << top) for t in (1, 2, 3)]
        low = jnp.concatenate([g[:, :chunk] for g in got], axis=1)
        norms = [from_parts(g[:, chunk:]) for g in got]
        norm_half = (norms[0] + norms[1]) + (norms[2] + norms[3])
        wide = low.astype(F32)
        sums = [norm_half, jnp.sum(wide * wide, axis=1, keepdims=True), jnp.sum(wide * direction, axis=1, keepdims=True)]
        part_own, part_far = dot_t(low, x_own), dot_t(low, x_far)
        sent = jnp.concatenate([part_own, part_far, jnp.pad(jnp.concatenate(sums, axis=1), ((0, 0), (0, LANES - 3)))], axis=1)
        back = swap(sent, count, 1)
        tail = sent[:, 2 * rows :] + back[:, 2 * rows :]
        norm_next, low_low, low_dir = tail[:, 0:1], tail[:, 1:2], tail[:, 2:3]
        image_own_new = mask_own * (part_own + back[:, rows : 2 * rows])
        image_far_new = mask_far * (part_far + back[:, :rows])
        if number == 0:
            direction, length = wide, low_low
            image_own, image_far = image_own_new, image_far_new
        else:
            beta = norm_next / norm_now
            direction = wide + beta * direction
            length = low_low + beta * (2.0 * low_dir + beta * length)
            image_own = image_own_new + beta * image_own
            image_far = image_far_new + beta * image_far
        norm_now = norm_next
        rounded_own, rounded_far = image_own.astype(BF16), image_far.astype(BF16)
        energy_own = jnp.sum(image_own * rounded_own.astype(F32), axis=1, keepdims=True)
        if number == ITERS - 1:
            break
        energy = energy_own + jnp.sum(image_far * rounded_far.astype(F32), axis=1, keepdims=True)
        sum_people = over_people(dot(rounded_own, x_own) + dot(rounded_far, x_far), energy, F32 if number == 0 else BF16)
        step = norm_now / (sum_people[:, chunk : chunk + 1] / noise_var + ridge * length)
        search = search - step * (sum_people[:, :chunk] / noise_var + ridge * direction[:, :chunk])
        batch_half = batch_half + step * direction
        fitted = fitted + step * image_own

    before = partial_res - fitted
    tails = [energy_own]
    tails += [jnp.sum(a * b, axis=1, keepdims=True) for a, b in ((before, before), (before, image_own), (image_own, image_own))]
    total = jnp.pad(jnp.concatenate(tails, axis=1), ((0, 0), (0, LANES - 4)))
    for bit in range(top):
        total = total + swap(total, count, 1 << bit)
    got = [total] + [swap(total, count, t << top) for t in (1, 2, 3)]
    total = (got[0] + got[1]) + (got[2] + got[3])
    step = norm_now / (total[:, 0:1] / noise_var + ridge * length)
    residual_new = before - step * image_own
    squares = total[:, 1] - step[:, 0] * (2.0 * total[:, 2] - step[:, 0] * total[:, 3])
    present = jnp.sum(valid_counts).astype(F32)
    sigma2_new = (squares + PRIOR_DOF * PRIOR_SCALE) / ((present + PRIOR_DOF) * gamma_draw)
    pair = jnp.concatenate([batch_half, direction], axis=1)
    pair_far = swap(pair, count, 1)
    coef_new = coef_all
    for side, both in ((core, pair), (1 - core, pair_far)):
        done = both[:, :half] + step * both[:, half:]
        for t in range(4):
            where = first_col + side * half + (place ^ t) * chunk
            coef_new = lax.dynamic_update_slice_in_dim(coef_new, done[:, t * chunk : (t + 1) * chunk], where, 1)
    return (coef_new, residual_new, sigma2_new)


def solution(mesh):
    return jax.shard_map(
        functools.partial(per_device, mesh.shape["ppl"]),
        mesh=mesh,
        in_specs=(
            P(("trait", "ppl"), None),
            P("trait", "ppl"),
            P("trait", "ppl"),
            P("trait", None),
            P("trait", None),
            P("trait"),
            P("trait"),
            P("trait"),
            P("trait"),
            P("trait"),
        ),
        out_specs=(P("trait", None), P("trait", "ppl"), P("trait")),
        check_vma=False,
    )
```

```python
import functools

import jax
import jax.numpy as jnp
from jax import lax
from jax.experimental import pallas as pl
from jax.experimental.pallas import tpu as pltpu
from jax.sharding import PartitionSpec as P


ITERS = 4
PRIOR_DOF = 4.0
PRIOR_SCALE = 0.5
CONTRACT = (((1,), (1,)), ((), ()))
LANES = 128
QUAD = 4
F32, BF16 = jnp.float32, jnp.bfloat16


def to_parts(value):
    first = lax.reduce_precision(value, 8, 7)
    second = lax.reduce_precision(value - first, 8, 7)
    third = value - first - second
    parts = jnp.concatenate([first, second, third], axis=1).astype(BF16)
    return jnp.pad(parts, ((0, 0), (0, LANES - 3)))


def from_parts(parts):
    wide = parts.astype(F32)
    return (wide[:, 2:3] + wide[:, 1:2]) + wide[:, 0:1]


def row_sum(values):
    return jnp.sum(values, axis=1, keepdims=True)


def by_pairs(terms):
    return (terms[0] + terms[1]) + (terms[2] + terms[3])


def lanes(columns):
    return jnp.pad(jnp.concatenate(columns, axis=1), ((0, 0), (0, LANES - len(columns))))


def per_device(
    count,
    genotypes,
    residual,
    noise_people,
    noise_coef,
    coef_all,
    block_index,
    prior_prec,
    sigma2_old,
    gamma_draw,
    valid_counts,
):
    rows, width = genotypes.shape
    traits = residual.shape[0]
    quarter = width // QUAD
    me = lax.axis_index("ppl")
    own = me & (QUAD - 1)
    dot_t = functools.partial(lax.dot_general, dimension_numbers=CONTRACT, preferred_element_type=F32)
    dot = functools.partial(jnp.dot, preferred_element_type=F32)

    def swap(x, distance):
        return lax.ppermute(x, "ppl", [(i, i ^ distance) for i in range(count)])

    def over_z(x, read=lambda piece: piece):
        stride = QUAD
        while stride < count:
            ways = (1, 2, 3) if stride * 4 <= count else (1,)
            got = [read(x)] + [read(swap(x, way * stride)) for way in ways]
            x = got[0] + got[1] if len(got) == 2 else (got[0] + got[1]) + (got[2] + got[3])
            stride *= len(got)
            read = lambda piece: piece
        return x

    def unpack(piece):
        scalar = jnp.broadcast_to(from_parts(piece[:, quarter:]), (traits, LANES))
        return jnp.concatenate([piece[:, :quarter].astype(F32), scalar], axis=1)

    def columns(array, slot):
        return lax.dynamic_slice_in_dim(array, (own ^ slot) * quarter, quarter, 1)

    x_give = [columns(genotypes, u) for u in range(QUAD)]
    slots = jnp.arange(rows)
    mask = [(slots < valid_counts[me ^ u]).astype(F32)[None, :] for u in range(QUAD)]
    first_col = block_index[0] * width
    noise_var = sigma2_old[:, None]
    ridge = prior_prec[:, None]

    old_coef = lax.dynamic_slice_in_dim(coef_all, first_col, width, 1)
    fitted_old = dot_t(old_coef.astype(BF16), genotypes)
    partial_res = mask[0] * (residual + fitted_old)
    target = (mask[0] * (partial_res + jnp.sqrt(noise_var) * noise_people)).astype(BF16)
    data = [dot(target, x_give[u]) for u in range(QUAD)]
    back = swap(jnp.concatenate([data[1], data[3]], axis=1), 1)
    kept, given = data[0] + back[:, :quarter], data[2] + back[:, quarter:]
    given, x_give = lax.optimization_barrier((given, x_give))
    kept = kept + swap(given, 2)
    x = [x_give[0]] + [swap(x_give[u], u) for u in (1, 2, 3)]
    kept = over_z(kept)
    search = kept / noise_var + jnp.sqrt(ridge) * columns(noise_coef, 0)

    image = direction = length = norm_now = None
    lows, mix, weights = [], [], []
    for number in range(ITERS):
        low = search.astype(BF16)
        lows.append(low)
        wide = low.astype(F32)
        sums = [row_sum(search * search), row_sum(wide * wide)]
        if number:
            sums.append(row_sum(wide * direction))
        sent = jnp.concatenate([dot_t(low, x[u]) for u in range(QUAD)] + [lanes(sums)], axis=1)
        for way in (1, 2):
            back = swap(sent, way)
            cuts = [back[:, (u ^ way) * rows : ((u ^ way) + 1) * rows] for u in range(QUAD)]
            sent = sent + jnp.concatenate(cuts + [back[:, QUAD * rows :]], axis=1)
        tail = sent[:, QUAD * rows :]
        fresh = [mask[u] * sent[:, u * rows : (u + 1) * rows] for u in range(QUAD)]
        norm_next = tail[:, 0:1]
        if number == 0:
            image, direction, length = fresh, wide, tail[:, 1:2]
        else:
            beta = norm_next / norm_now
            image = [new + beta * old for new, old in zip(fresh, image)]
            direction = wide + beta * direction
            length = tail[:, 1:2] + beta * (2.0 * tail[:, 2:3] + beta * length)
            mix = [beta * m for m in mix]
        mix.append(jnp.ones_like(norm_next))
        weights.append(jnp.zeros_like(norm_next))
        norm_now = norm_next
        rounded = [value.astype(BF16) for value in image]
        energy = by_pairs([row_sum(a * b.astype(F32)) for a, b in zip(image, rounded)])
        if number == ITERS - 1:
            break
        part = sum(dot(rounded[u], x[u]) for u in range(QUAD))
        if number == 0:
            total = over_z(jnp.concatenate([part, jnp.broadcast_to(energy, (traits, LANES))], axis=1))
        else:
            total = over_z(jnp.concatenate([part.astype(BF16), to_parts(energy)], axis=1), unpack)
        if number == 0:
            before = [partial_res] + [swap(partial_res, u) for u in (1, 2, 3)]
            total, before = lax.optimization_barrier((total, before))
        if number == ITERS - 2:
            early = jnp.concatenate(lows, axis=1)
            early = [early] + [swap(early, u) for u in (1, 2, 3)]
            total, early = lax.optimization_barrier((total, early))
        step = norm_now / (total[:, quarter : quarter + 1] / noise_var + ridge * length)
        search = search - step * (total[:, :quarter] / noise_var + ridge * direction)
        before = [a - step * b for a, b in zip(before, image)]
        weights = [w + step * m for w, m in zip(weights, mix)]

    late = [lows[-1]] + [swap(lows[-1], u) for u in (1, 2, 3)]
    pairs = zip(before, image)
    products = [[row_sum(a * a), row_sum(a * b), row_sum(b * b)] for a, b in pairs]
    total = over_z(lanes([energy] + [by_pairs(column) for column in zip(*products)]))
    step = norm_now / (total[:, 0:1] / noise_var + ridge * length)
    residual_new = before[0] - step * image[0]
    squares = total[:, 1] - step[:, 0] * (2.0 * total[:, 2] - step[:, 0] * total[:, 3])
    present = jnp.sum(valid_counts).astype(F32)
    sigma2_new = (squares + PRIOR_DOF * PRIOR_SCALE) / ((present + PRIOR_DOF) * gamma_draw)
    weights = lanes([w + step * m for w, m in zip(weights, mix)])
    coef_new = write_coef(jnp.stack([block_index[0], own]).astype(jnp.int32), weights, early, late, coef_all)
    return (coef_new, residual_new, sigma2_new)


def write_coef(where, weights, early, late, coef_all):
    traits, quarter = late[0].shape
    width = QUAD * quarter
    blocks = coef_all.shape[1] // width
    kept = ITERS - 1

    def kernel(where_ref, weights_ref, *refs):
        early_refs, late_refs = refs[:QUAD], refs[QUAD : 2 * QUAD]
        coef_ref, out_ref, scratch, sems = refs[2 * QUAD :]
        block = where_ref[0]

        def hold(index):
            span = pl.ds(index * width, width)
            return pltpu.make_async_copy(coef_ref.at[:, span], out_ref.at[:, span], sems.at[index])

        def give(slot):
            start = pl.multiple_of(block * width + (where_ref[1] ^ slot) * quarter, LANES)
            return pltpu.make_async_copy(scratch.at[slot], out_ref.at[:, pl.ds(start, quarter)], sems.at[blocks + slot])

        for index in range(blocks):
            pl.when(block != index)(lambda index=index: hold(index).start())
        scale = [weights_ref[:, k : k + 1] for k in range(ITERS)]
        for slot in range(QUAD):
            value = scale[kept] * late_refs[slot][...].astype(F32)
            for k in range(kept):
                value += scale[k] * early_refs[slot][:, k * quarter : (k + 1) * quarter].astype(F32)
            scratch[slot] = value
            give(slot).start()
        for slot in range(QUAD):
            give(slot).wait()
        for index in range(blocks):
            pl.when(block != index)(lambda index=index: hold(index).wait())

    vmem = pl.BlockSpec(memory_space=pltpu.VMEM)
    return pl.pallas_call(
        kernel,
        out_shape=jax.ShapeDtypeStruct(coef_all.shape, coef_all.dtype),
        in_specs=[pl.BlockSpec(memory_space=pltpu.SMEM)] + [vmem] * (1 + 2 * QUAD) + [pl.BlockSpec(memory_space=pl.ANY)],
        out_specs=pl.BlockSpec(memory_space=pl.ANY),
        scratch_shapes=[pltpu.VMEM((QUAD, traits, quarter), F32), pltpu.SemaphoreType.DMA((blocks + QUAD,))],
    )(where, weights, *early, *late, coef_all)


def solution(mesh):
    return jax.shard_map(
        functools.partial(per_device, mesh.shape["ppl"]),
        mesh=mesh,
        in_specs=(
            P(("trait", "ppl"), None),
            P("trait", "ppl"),
            P("trait", "ppl"),
            P("trait", None),
            P("trait", None),
            P("trait"),
            P("trait"),
            P("trait"),
            P("trait"),
            P("trait"),
        ),
        out_specs=(P("trait", None), P("trait", "ppl"), P("trait")),
        check_vma=False,
    )
```

```python
import functools

import jax
import jax.numpy as jnp
from jax import lax
from jax.experimental import pallas as pl
from jax.experimental.pallas import tpu as pltpu
from jax.sharding import PartitionSpec as P


ITERS = 4
PRIOR_DOF = 4.0
PRIOR_SCALE = 0.5
LANES = 128
TILE = 8
QUAD = 4
F32, BF16 = jnp.float32, jnp.bfloat16
PEOPLE_KIND = (F32, BF16, BF16)
IMAGE_KIND = (F32, BF16, BF16, BF16)
VMEM = pl.BlockSpec(memory_space=pltpu.VMEM)
SMEM = pl.BlockSpec(memory_space=pltpu.SMEM)
ANY = pl.BlockSpec(memory_space=pl.ANY)


def dot(a, b):
    return lax.dot_general(a, b, (((1,), (0,)), ((), ())), preferred_element_type=F32)


def dot_t(a, b):
    return lax.dot_general(a, b, (((1,), (1,)), ((), ())), preferred_element_type=F32)


def row_sum(values):
    return jnp.sum(values, axis=1, keepdims=True)


def by_pairs(terms):
    return (terms[0] + terms[1]) + (terms[2] + terms[3])


def diagonal(shape):
    return lax.broadcasted_iota(jnp.int32, shape, 0) == lax.broadcasted_iota(jnp.int32, shape, 1)


def to_row(column):
    same = diagonal((column.shape[0], LANES))
    return jnp.sum(jnp.where(same, column, 0.0), axis=0, keepdims=True)


def to_column(row, traits):
    same = diagonal((traits, row.shape[1]))
    return jnp.sum(jnp.where(same, row, 0.0), axis=1, keepdims=True)


def parts_of(value, kind):
    if kind == F32:
        return [value]
    first = value.astype(BF16)
    rest = value - first.astype(F32)
    second = rest.astype(BF16)
    return [first.astype(F32), second.astype(F32), rest - second.astype(F32)]


def pack(wide, columns, kind):
    _, width = wide.shape
    blocks = [wide[:, at : at + LANES].astype(kind) for at in range(0, width, LANES)]
    rows = [part for column in columns for part in parts_of(to_row(column), kind)]
    if rows:
        pad = -len(rows) % TILE
        rows.append(jnp.zeros((pad, LANES), F32))
        blocks.append(jnp.concatenate(rows, axis=0).astype(kind))
    return jnp.concatenate(blocks, axis=0)


def unpack(packed, traits, width, count=0):
    lines = traits * width // LANES
    wide = jnp.concatenate([packed[at : at + traits].astype(F32) for at in range(0, lines, traits)], axis=1)
    per = 1 if packed.dtype == F32 else 3
    rows = packed[lines:].astype(F32)
    columns = []
    for index in range(count):
        mine = [rows[index * per + k : index * per + k + 1] for k in range(per)]
        row = mine[0] if per == 1 else (mine[2] + mine[1]) + mine[0]
        columns.append(to_column(row, traits))
    return wide, columns


def fuse(fn, *args):
    shapes = jax.eval_shape(fn, *args)

    def kernel(*refs):
        ins, outs = refs[: len(args)], refs[len(args) :]
        for out, value in zip(outs, fn(*(ref[...] for ref in ins))):
            out[...] = value

    return pl.pallas_call(kernel, out_shape=shapes, in_specs=[VMEM] * len(args), out_specs=[VMEM] * len(shapes))(*args)


def prepare(where, genotypes, coef_all, noise_coef, residual, noise_people, mask, sigma2_old, prior_prec):
    rows, width = genotypes.shape
    traits = residual.shape[0]
    quarter = width // QUAD

    def kernel(where_ref, geno_ref, coef_ref, noise_ref, res_ref, people_ref, mask_ref, sigma_ref, prior_ref, *refs):
        x_refs, (noise_out, partial_ref, kept_ref, given_ref, cross_ref, var_ref, ridge_ref, old_ref, sems) = refs[:QUAD], refs[QUAD:]
        copies = []
        for slot in range(QUAD):
            start = pl.multiple_of((where_ref[1] ^ slot) * quarter, LANES)
            first = pl.multiple_of(where_ref[0] * width + start, LANES)
            pair = (
                pltpu.make_async_copy(coef_ref.at[:, pl.ds(first, quarter)], old_ref.at[slot], sems.at[2 * slot]),
                pltpu.make_async_copy(geno_ref.at[:, pl.ds(start, quarter)], x_refs[slot], sems.at[2 * slot + 1]),
            )
            for copy in pair:
                copy.start()
            copies.append(pair)
        start = pl.multiple_of(where_ref[1] * quarter, LANES)
        last = pltpu.make_async_copy(noise_ref.at[:, pl.ds(start, quarter)], noise_out, sems.at[2 * QUAD])
        last.start()
        noise_var = to_column(sigma_ref[...], traits)
        var_ref[...] = noise_var
        ridge_ref[...] = to_column(prior_ref[...], traits)
        fitted = jnp.zeros((traits, rows), F32)
        for slot in range(QUAD):
            for copy in copies[slot]:
                copy.wait()
            fitted += dot_t(old_ref[slot].astype(BF16), x_refs[slot][...])
        present = mask_ref[0:1]
        partial = present * (res_ref[...] + fitted)
        partial_ref[...] = partial
        target = (present * (partial + jnp.sqrt(noise_var) * people_ref[...])).astype(BF16)
        lines = traits * quarter // LANES
        cross_ref[:lines] = pack(dot(target, x_refs[1][...]), (), F32)
        cross_ref[lines:] = pack(dot(target, x_refs[3][...]), (), F32)
        given_ref[...] = pack(dot(target, x_refs[2][...]), (), F32)
        kept_ref[...] = pack(dot(target, x_refs[0][...]), (), F32)
        last.wait()

    lines = traits * quarter // LANES
    shape = jax.ShapeDtypeStruct
    out_shape = [shape((rows, quarter), BF16)] * QUAD + [
        shape((traits, quarter), F32),
        shape((traits, rows), F32),
        shape((lines, LANES), F32),
        shape((lines, LANES), F32),
        shape((2 * lines, LANES), F32),
        shape((traits, 1), F32),
        shape((traits, 1), F32),
    ]
    return pl.pallas_call(
        kernel,
        out_shape=out_shape,
        in_specs=[SMEM, ANY, ANY, ANY] + [VMEM] * 5,
        out_specs=[VMEM] * len(out_shape),
        scratch_shapes=[pltpu.VMEM((QUAD, traits, quarter), F32), pltpu.SemaphoreType.DMA((2 * QUAD + 1,))],
    )(where, genotypes, coef_all, noise_coef, residual, noise_people, mask, sigma2_old, prior_prec)


def image_part(search, direction, x):
    low = search.astype(BF16)
    wide = low.astype(F32)
    sums = [row_sum(search * search), row_sum(wide * wide)]
    if direction is not None:
        sums.append(row_sum(wide * direction))
    image = jnp.concatenate([dot_t(low, block) for block in x], axis=1)
    return pack(image, sums, F32), search, low


def first_search(got0, got1, got2, got3, noise_coef, noise_var, ridge, *x):
    traits, quarter = noise_coef.shape
    total, _ = unpack((got0 + got1) + (got2 + got3), traits, quarter)
    return image_part(total / noise_var + jnp.sqrt(ridge) * noise_coef, None, x)


def next_search(got0, got1, got2, got3, search, direction, image, before, norm, length, noise_var, ridge, *x):
    traits, quarter = search.shape
    opened = [unpack(got, traits, quarter, 1) for got in (got0, got1, got2, got3)]
    total = by_pairs([wide for wide, _ in opened])
    energy = by_pairs([columns[0] for _, columns in opened])
    step = norm / (energy / noise_var + ridge * length)
    search = search - step * (total / noise_var + ridge * direction)
    return *image_part(search, direction, x), before - step * image, step


def cross(packed, way, traits, rows):
    lines = traits * rows // LANES
    blocks = [packed[(slot ^ way) * lines : ((slot ^ way) + 1) * lines] for slot in range(QUAD)]
    return jnp.concatenate(blocks + [packed[QUAD * lines :]], axis=0)


def over_core(kind, count, traits, rows, sent, back):
    total = sent + cross(back, 1, traits, rows)
    if kind == F32:
        return (total,)
    wide, columns = unpack(total, traits, QUAD * rows, count)
    return (pack(wide, columns, kind),)


def new_image(count, sent, back, mask, low, direction, image, norm_old, length):
    traits = low.shape[0]
    rows = mask.shape[1]
    wide, columns = unpack(sent, traits, QUAD * rows, count)
    far, far_columns = unpack(cross(back, 2, traits, rows), traits, QUAD * rows, count)
    columns = [a + b for a, b in zip(columns, far_columns)]
    present = jnp.concatenate([mask[slot : slot + 1] for slot in range(QUAD)], axis=1)
    fresh = present * (wide + far)
    norm, low_low = columns[:2]
    wide = low.astype(F32)
    if direction is None:
        return fresh, wide, norm, low_low, jnp.zeros_like(norm)
    beta = norm / norm_old
    length = low_low + beta * (2.0 * columns[2] + beta * length)
    return fresh + beta * image, wide + beta * direction, norm, length, beta


def slots_of(wide, rows):
    return [wide[:, slot * rows : (slot + 1) * rows] for slot in range(QUAD)]


def people_part(kind, first, sent, back, mask, low, *rest):
    if first:
        state, x = new_image(2, sent, back, mask, low, None, None, None, None), rest
    else:
        state, x = new_image(3, sent, back, mask, low, *rest[:4]), rest[4:]
    rounded = state[0].astype(BF16)
    rows = mask.shape[1]
    energy = by_pairs([row_sum(part) for part in slots_of(state[0] * rounded.astype(F32), rows)])
    total = by_pairs([dot(part, block) for part, block in zip(slots_of(rounded, rows), x)])
    return pack(total, [energy], kind), *state


def last_sums(sent, back, mask, low, direction, image, norm_old, length, before):
    image, _, norm, length, beta = new_image(3, sent, back, mask, low, direction, image, norm_old, length)
    rows = mask.shape[1]
    products = (image * image.astype(BF16).astype(F32), before * before, before * image, image * image)
    sums = [to_row(by_pairs([row_sum(part) for part in slots_of(product, rows)])) for product in products]
    packed = jnp.concatenate(sums + [jnp.zeros((TILE - len(sums), LANES), F32)], axis=0)
    return packed, image[:, :rows], norm, length, beta


def finish(where, got, norm, length, noise_var, ridge, gamma, before, image, steps, betas, early, late, coef_all):
    traits, quarter = late[0].shape
    rows = image.shape[1]
    width = QUAD * quarter
    blocks = coef_all.shape[1] // width
    kept = ITERS - 1
    args = [*got, norm, length, noise_var, ridge, gamma, before, image, *steps, *betas, *early, *late]
    split = [len(got), 7, kept, kept, QUAD, QUAD]

    def kernel(where_ref, *refs):
        groups, at = [], 0
        for size in split:
            groups.append(refs[at : at + size])
            at += size
        coef_ref, out_ref, res_ref, sigma_ref, scratch, sems = refs[at:]
        block = where_ref[0]

        def hold(index):
            span = pl.ds(index * width, width)
            return pltpu.make_async_copy(coef_ref.at[:, span], out_ref.at[:, span], sems.at[index])

        def give(slot):
            start = pl.multiple_of(block * width + (where_ref[1] ^ slot) * quarter, LANES)
            return pltpu.make_async_copy(scratch.at[slot], out_ref.at[:, pl.ds(start, quarter)], sems.at[blocks + slot])

        for index in range(blocks):
            pl.when(block != index)(lambda index=index: hold(index).start())
        got, (norm, length, noise_var, ridge, gamma, before, image), steps, betas, early, late = groups
        total = by_pairs([ref[...] for ref in got]) if len(got) == QUAD else got[0][...]
        energy, squares, mixed, energy_full = (to_column(total[k : k + 1], traits) for k in range(4))
        step = norm[...] / (energy / noise_var[...] + ridge[...] * length[...])
        scale, mix = [], []
        for number in range(ITERS):
            mix = [betas[number - 1][...] * m for m in mix] + [jnp.ones_like(step)]
            now = steps[number][...] if number < kept else step
            scale = [s + now * m for s, m in zip(scale + [jnp.zeros_like(step)], mix)]
        for slot in range(QUAD):
            value = scale[kept] * late[slot][...].astype(F32)
            for k in range(kept):
                value += scale[k] * early[slot][k * traits : (k + 1) * traits].astype(F32)
            scratch[slot] = value
            give(slot).start()
        res_ref[...] = before[:, :rows] - step * image[...]
        squares = squares - step * (2.0 * mixed - step * energy_full)
        present = where_ref[2].astype(F32)
        row = to_row(squares + PRIOR_DOF * PRIOR_SCALE)[:, :traits]
        sigma_ref[...] = row / ((present + PRIOR_DOF) * gamma[...])
        for slot in range(QUAD):
            give(slot).wait()
        for index in range(blocks):
            pl.when(block != index)(lambda index=index: hold(index).wait())

    shape = jax.ShapeDtypeStruct
    return pl.pallas_call(
        kernel,
        out_shape=[shape(coef_all.shape, F32), shape((traits, rows), F32), shape((1, traits), F32)],
        in_specs=[SMEM] + [VMEM] * (len(args) + 1),
        out_specs=[ANY, VMEM, VMEM],
        scratch_shapes=[pltpu.VMEM((QUAD, traits, quarter), F32), pltpu.SemaphoreType.DMA((blocks + QUAD,))],
    )(where, *args, coef_all)


def per_device(
    count,
    genotypes,
    residual,
    noise_people,
    noise_coef,
    coef_all,
    block_index,
    prior_prec,
    sigma2_old,
    gamma_draw,
    valid_counts,
):
    rows, width = genotypes.shape
    traits = residual.shape[0]
    quarter = width // QUAD
    me = lax.axis_index("ppl")
    own = me & (QUAD - 1)

    def swap(x, distance):
        return lax.ppermute(x, "ppl", [(i, i ^ distance) for i in range(count)])

    def share(x):
        return [x] + [swap(x, slot) for slot in (1, 2, 3)]

    def over_z(x, columns):
        stride, kind = QUAD, x.dtype
        while True:
            got = [x] + [swap(x, way * stride) for way in (1, 2, 3)]
            stride *= 4
            if stride >= count:
                return got

            def add(*got):
                opened = [unpack(piece, traits, quarter, columns) for piece in got]
                sums = [by_pairs(list(column)) for column in zip(*(c for _, c in opened))]
                return (pack(by_pairs([wide for wide, _ in opened]), sums, kind),)

            if x.shape[0] == TILE:
                x = by_pairs(got)
            else:
                (x,) = fuse(add, *got)

    slots = jnp.arange(rows)
    quad = valid_counts[jnp.bitwise_xor(me, jnp.arange(QUAD))]
    mask = (slots[None, :] < quad[:, None]).astype(F32)
    where = jnp.stack([block_index[0], own, jnp.sum(valid_counts)]).astype(jnp.int32)
    made = prepare(
        where, genotypes, coef_all, noise_coef, residual, noise_people, mask, sigma2_old.reshape(1, -1), prior_prec.reshape(1, -1)
    )
    x_give, (noise_quarter, partial_res, kept, given, sent, noise_var, ridge) = made[:QUAD], made[QUAD:]
    lines = kept.shape[0]
    back = swap(sent, 1)
    given = given + back[lines:]
    given, x_give = lax.optimization_barrier((given, x_give))
    kept = kept + back[:lines] + swap(given, 2)
    x = [x_give[0]] + [swap(x_give[slot], slot) for slot in (1, 2, 3)]
    got = over_z(kept, 0)

    steps, betas, lows = [], [], []
    for number in range(ITERS):
        if number == 0:
            sent, search, low = fuse(first_search, *got, noise_quarter, noise_var, ridge, *x)
        else:
            sent, search, low, before, step = fuse(
                next_search, *got, search, direction, image, before, norm, length, noise_var, ridge, *x
            )
            steps.append(step)
        lows.append(low)
        (sent,) = fuse(functools.partial(over_core, IMAGE_KIND[number], 3 if number else 2, traits, rows), sent, swap(sent, 1))
        back = swap(sent, 2)
        if number == ITERS - 1:
            sent, image, norm, length, beta = fuse(last_sums, sent, back, mask, low, direction, image, norm, length, before)
            betas.append(beta)
            break
        state = (direction, image, norm, length) if number else ()
        sent, image, direction, norm, length, beta = fuse(
            functools.partial(people_part, PEOPLE_KIND[number], number == 0), sent, back, mask, low, *state, *x
        )
        if number:
            betas.append(beta)
        got = over_z(sent, 1)
        if number == 0:
            before = share(partial_res)
            got, before = lax.optimization_barrier((got, before))
            before = jnp.concatenate(before, axis=1)
        if number == ITERS - 2:
            early = share(jnp.concatenate(lows, axis=0))
            got, early = lax.optimization_barrier((got, early))

    late = share(low)
    got = over_z(sent, 4)
    coef_new, residual_new, sigma2_new = finish(
        where, got, norm, length, noise_var, ridge, gamma_draw.reshape(1, -1), before, image, steps, betas, early, late, coef_all
    )
    return (coef_new, residual_new, sigma2_new.reshape(-1))


def solution(mesh):
    return jax.shard_map(
        functools.partial(per_device, mesh.shape["ppl"]),
        mesh=mesh,
        in_specs=(
            P(("trait", "ppl"), None),
            P("trait", "ppl"),
            P("trait", "ppl"),
            P("trait", None),
            P("trait", None),
            P("trait"),
            P("trait"),
            P("trait"),
            P("trait"),
            P("trait"),
        ),
        out_specs=(P("trait", None), P("trait", "ppl"), P("trait")),
        check_vma=False,
    )
```

```python
import functools

import jax
import jax.numpy as jnp
from jax import lax
from jax.experimental import pallas as pl
from jax.experimental.pallas import tpu as pltpu
from jax.sharding import PartitionSpec as P


ITERS = 4
PRIOR_DOF = 4.0
PRIOR_SCALE = 0.5
LANES = 128
TILE = 8
QUAD = 4
F32, BF16 = jnp.float32, jnp.bfloat16
PEOPLE_KIND = (F32, BF16, BF16)
IMAGE_KIND = (F32, BF16, BF16, BF16)
VMEM = pl.BlockSpec(memory_space=pltpu.VMEM)
SMEM = pl.BlockSpec(memory_space=pltpu.SMEM)
ANY = pl.BlockSpec(memory_space=pl.ANY)
PARAMS = pltpu.CompilerParams(vmem_limit_bytes=12 << 20)


def dot(a, b):
    return lax.dot_general(a, b, (((1,), (0,)), ((), ())), preferred_element_type=F32)


def dot_t(a, b):
    return lax.dot_general(a, b, (((1,), (1,)), ((), ())), preferred_element_type=F32)


def row_sum(values):
    return jnp.sum(values, axis=1, keepdims=True)


def by_pairs(terms):
    return (terms[0] + terms[1]) + (terms[2] + terms[3])


def diagonal(shape):
    return lax.broadcasted_iota(jnp.int32, shape, 0) == lax.broadcasted_iota(jnp.int32, shape, 1)


def to_row(column):
    same = diagonal((column.shape[0], LANES))
    return jnp.sum(jnp.where(same, column, 0.0), axis=0, keepdims=True)


def to_column(row, traits):
    same = diagonal((traits, row.shape[1]))
    return jnp.sum(jnp.where(same, row, 0.0), axis=1, keepdims=True)


def parts_of(value, kind):
    if kind == F32:
        return [value]
    first = value.astype(BF16)
    rest = value - first.astype(F32)
    second = rest.astype(BF16)
    return [first.astype(F32), second.astype(F32), rest - second.astype(F32)]


def pack(wide, columns, kind):
    _, width = wide.shape
    blocks = [wide[:, at : at + LANES].astype(kind) for at in range(0, width, LANES)]
    rows = [part for column in columns for part in parts_of(to_row(column), kind)]
    if rows:
        pad = -len(rows) % TILE
        rows.append(jnp.zeros((pad, LANES), F32))
        blocks.append(jnp.concatenate(rows, axis=0).astype(kind))
    return jnp.concatenate(blocks, axis=0)


def unpack(packed, traits, width, count=0):
    lines = traits * width // LANES
    wide = jnp.concatenate([packed[at : at + traits].astype(F32) for at in range(0, lines, traits)], axis=1)
    per = 1 if packed.dtype == F32 else 3
    rows = packed[lines:].astype(F32)
    columns = []
    for index in range(count):
        mine = [rows[index * per + k : index * per + k + 1] for k in range(per)]
        row = mine[0] if per == 1 else (mine[2] + mine[1]) + mine[0]
        columns.append(to_column(row, traits))
    return wide, columns


def fuse(fn, *args):
    shapes = jax.eval_shape(fn, *args)

    def kernel(*refs):
        ins, outs = refs[: len(args)], refs[len(args) :]
        for out, value in zip(outs, fn(*(ref[...] for ref in ins))):
            out[...] = value

    return pl.pallas_call(kernel, out_shape=shapes, compiler_params=PARAMS, in_specs=[VMEM] * len(args), out_specs=[VMEM] * len(shapes))(*args)


def place_in_quad():
    return lax.axis_index("ppl") & (QUAD - 1)


def prepare(block_index, valid_counts, genotypes, coef_all, noise_coef, residual, noise_people, sigma2_old, prior_prec):
    rows, width = genotypes.shape
    traits = residual.shape[0]
    quarter = width // QUAD

    def kernel(block_ref, valid_ref, geno_ref, coef_ref, noise_ref, res_ref, people_ref, sigma_ref, prior_ref, *refs):
        x_refs, refs = refs[:QUAD], refs[QUAD:]
        noise_out, partial_ref, kept_ref, given_ref, cross_ref, var_ref, ridge_ref, mask_ref, old_ref, sems = refs
        me = lax.axis_index("ppl")
        own = place_in_quad()
        copies = []
        for slot in range(QUAD):
            start = pl.multiple_of((own ^ slot) * quarter, LANES)
            first = pl.multiple_of(block_ref[0] * width + start, LANES)
            pair = (
                pltpu.make_async_copy(coef_ref.at[:, pl.ds(first, quarter)], old_ref.at[slot], sems.at[2 * slot]),
                pltpu.make_async_copy(geno_ref.at[:, pl.ds(start, quarter)], x_refs[slot], sems.at[2 * slot + 1]),
            )
            for copy in pair:
                copy.start()
            copies.append(pair)
        start = pl.multiple_of(own * quarter, LANES)
        last = pltpu.make_async_copy(noise_ref.at[:, pl.ds(start, quarter)], noise_out, sems.at[2 * QUAD])
        last.start()
        noise_var = to_column(sigma_ref[...], traits)
        var_ref[...] = noise_var
        ridge_ref[...] = to_column(prior_ref[...], traits)
        fitted = jnp.zeros((traits, rows), F32)
        for slot in range(QUAD):
            for copy in copies[slot]:
                copy.wait()
            fitted += dot_t(old_ref[slot].astype(BF16), x_refs[slot][...])
        slots = lax.broadcasted_iota(jnp.int32, (1, rows), 1)
        for slot in range(QUAD):
            mask_ref[:, slot * rows : (slot + 1) * rows] = (slots < valid_ref[me ^ slot]).astype(F32)
        present = (slots < valid_ref[me]).astype(F32)
        partial = present * (res_ref[...] + fitted)
        partial_ref[...] = partial
        target = (present * (partial + jnp.sqrt(noise_var) * people_ref[...])).astype(BF16)
        lines = traits * quarter // LANES
        cross_ref[:lines] = pack(dot(target, x_refs[1][...]), (), F32)
        cross_ref[lines:] = pack(dot(target, x_refs[3][...]), (), F32)
        given_ref[...] = pack(dot(target, x_refs[2][...]), (), F32)
        kept_ref[...] = pack(dot(target, x_refs[0][...]), (), F32)
        last.wait()

    lines = traits * quarter // LANES
    shape = jax.ShapeDtypeStruct
    out_shape = [shape((rows, quarter), BF16)] * QUAD + [
        shape((traits, quarter), F32),
        shape((traits, rows), F32),
        shape((lines, LANES), F32),
        shape((lines, LANES), F32),
        shape((2 * lines, LANES), F32),
        shape((traits, 1), F32),
        shape((traits, 1), F32),
        shape((1, QUAD * rows), F32),
    ]
    return pl.pallas_call(
        kernel,
        compiler_params=PARAMS,
        out_shape=out_shape,
        in_specs=[SMEM, SMEM, ANY, ANY, ANY] + [VMEM] * 4,
        out_specs=[VMEM] * len(out_shape),
        scratch_shapes=[pltpu.VMEM((QUAD, traits, quarter), F32), pltpu.SemaphoreType.DMA((2 * QUAD + 1,))],
    )(block_index, valid_counts, genotypes, coef_all, noise_coef, residual, noise_people, sigma2_old, prior_prec)


def image_part(search, direction, x):
    low = search.astype(BF16)
    wide = low.astype(F32)
    sums = [row_sum(search * search), row_sum(wide * wide)]
    if direction is not None:
        sums.append(row_sum(wide * direction))
    image = jnp.concatenate([dot_t(low, block) for block in x], axis=1)
    return pack(image, sums, F32), search, low


def first_search(got0, got1, got2, got3, noise_coef, noise_var, ridge, *x):
    traits, quarter = noise_coef.shape
    total, _ = unpack((got0 + got1) + (got2 + got3), traits, quarter)
    return image_part(total / noise_var + jnp.sqrt(ridge) * noise_coef, None, x)


def next_search(got0, got1, got2, got3, search, direction, image, before, norm, length, noise_var, ridge, *x):
    traits, quarter = search.shape
    opened = [unpack(got, traits, quarter, 1) for got in (got0, got1, got2, got3)]
    total = by_pairs([wide for wide, _ in opened])
    energy = by_pairs([columns[0] for _, columns in opened])
    step = norm / (energy / noise_var + ridge * length)
    search = search - step * (total / noise_var + ridge * direction)
    return *image_part(search, direction, x), before - step * image, step


def cross(packed, way, traits, rows):
    lines = traits * rows // LANES
    blocks = [packed[(slot ^ way) * lines : ((slot ^ way) + 1) * lines] for slot in range(QUAD)]
    return jnp.concatenate(blocks + [packed[QUAD * lines :]], axis=0)


def over_core(kind, count, traits, rows, sent, back):
    total = sent + cross(back, 1, traits, rows)
    if kind == F32:
        return (total,)
    wide, columns = unpack(total, traits, QUAD * rows, count)
    return (pack(wide, columns, kind),)


def new_image(count, sent, back, mask, low, direction, image, norm_old, length):
    traits = low.shape[0]
    rows = mask.shape[1] // QUAD
    wide, columns = unpack(sent, traits, QUAD * rows, count)
    far, far_columns = unpack(cross(back, 2, traits, rows), traits, QUAD * rows, count)
    columns = [a + b for a, b in zip(columns, far_columns)]
    fresh = mask * (wide + far)
    norm, low_low = columns[:2]
    wide = low.astype(F32)
    if direction is None:
        return fresh, wide, norm, low_low, jnp.zeros_like(norm)
    beta = norm / norm_old
    length = low_low + beta * (2.0 * columns[2] + beta * length)
    return fresh + beta * image, wide + beta * direction, norm, length, beta


def slots_of(wide, rows):
    return [wide[:, slot * rows : (slot + 1) * rows] for slot in range(QUAD)]


def people_part(kind, first, sent, back, mask, low, *rest):
    if first:
        state, x = new_image(2, sent, back, mask, low, None, None, None, None), rest
    else:
        state, x = new_image(3, sent, back, mask, low, *rest[:4]), rest[4:]
    rounded = state[0].astype(BF16)
    rows = mask.shape[1] // QUAD
    energy = by_pairs([row_sum(part) for part in slots_of(state[0] * rounded.astype(F32), rows)])
    total = by_pairs([dot(part, block) for part, block in zip(slots_of(rounded, rows), x)])
    return pack(total, [energy], kind), *state


def last_sums(sent, back, mask, low, direction, image, norm_old, length, before):
    image, _, norm, length, beta = new_image(3, sent, back, mask, low, direction, image, norm_old, length)
    rows = mask.shape[1] // QUAD
    products = (image * image.astype(BF16).astype(F32), before * before, before * image, image * image)
    sums = [to_row(by_pairs([row_sum(part) for part in slots_of(product, rows)])) for product in products]
    packed = jnp.concatenate(sums + [jnp.zeros((TILE - len(sums), LANES), F32)], axis=0)
    return packed, image[:, :rows], norm, length, beta


def finish(block_index, valid_counts, got, norm, length, noise_var, ridge, gamma, before, image, steps, betas, early, late, coef_all):
    traits, quarter = late[0].shape
    rows = image.shape[1]
    width = QUAD * quarter
    blocks = coef_all.shape[1] // width
    kept = ITERS - 1
    args = [*got, norm, length, noise_var, ridge, gamma, before, image, *steps, *betas, *early, *late]
    split = [len(got), 7, kept, kept, QUAD, QUAD]

    def kernel(block_ref, valid_ref, *refs):
        groups, at = [], 0
        for size in split:
            groups.append(refs[at : at + size])
            at += size
        coef_ref, out_ref, res_ref, sigma_ref, scratch, sems = refs[at:]
        block, own = block_ref[0], place_in_quad()

        def hold(index):
            span = pl.ds(index * width, width)
            return pltpu.make_async_copy(coef_ref.at[:, span], out_ref.at[:, span], sems.at[index])

        def give(slot):
            start = pl.multiple_of(block * width + (own ^ slot) * quarter, LANES)
            return pltpu.make_async_copy(scratch.at[slot], out_ref.at[:, pl.ds(start, quarter)], sems.at[blocks + slot])

        for index in range(blocks):
            pl.when(block != index)(lambda index=index: hold(index).start())
        got, (norm, length, noise_var, ridge, gamma, before, image), steps, betas, early, late = groups
        total = by_pairs([ref[...] for ref in got]) if len(got) == QUAD else got[0][...]
        energy, squares, mixed, energy_full = (to_column(total[k : k + 1], traits) for k in range(4))
        step = norm[...] / (energy / noise_var[...] + ridge[...] * length[...])
        scale, mix = [], []
        for number in range(ITERS):
            mix = [betas[number - 1][...] * m for m in mix] + [jnp.ones_like(step)]
            now = steps[number][...] if number < kept else step
            scale = [s + now * m for s, m in zip(scale + [jnp.zeros_like(step)], mix)]
        for slot in range(QUAD):
            value = scale[kept] * late[slot][...].astype(F32)
            for k in range(kept):
                value += scale[k] * early[slot][k * traits : (k + 1) * traits].astype(F32)
            scratch[slot] = value
            give(slot).start()
        res_ref[...] = before[:, :rows] - step * image[...]
        squares = squares - step * (2.0 * mixed - step * energy_full)
        present = sum(valid_ref[k] for k in range(valid_counts.shape[0])).astype(F32)
        row = to_row(squares + PRIOR_DOF * PRIOR_SCALE)[:, :traits]
        sigma_ref[...] = row / ((present + PRIOR_DOF) * gamma[...])
        for slot in range(QUAD):
            give(slot).wait()
        for index in range(blocks):
            pl.when(block != index)(lambda index=index: hold(index).wait())

    shape = jax.ShapeDtypeStruct
    return pl.pallas_call(
        kernel,
        compiler_params=PARAMS,
        out_shape=[shape(coef_all.shape, F32), shape((traits, rows), F32), shape((1, traits), F32)],
        in_specs=[SMEM, SMEM] + [VMEM] * (len(args) + 1),
        out_specs=[ANY, VMEM, VMEM],
        scratch_shapes=[pltpu.VMEM((QUAD, traits, quarter), F32), pltpu.SemaphoreType.DMA((blocks + QUAD,))],
    )(block_index, valid_counts, *args, coef_all)


def per_device(
    count,
    genotypes,
    residual,
    noise_people,
    noise_coef,
    coef_all,
    block_index,
    prior_prec,
    sigma2_old,
    gamma_draw,
    valid_counts,
):
    rows, width = genotypes.shape
    traits = residual.shape[0]
    quarter = width // QUAD

    def swap(x, distance):
        return lax.ppermute(x, "ppl", [(i, i ^ distance) for i in range(count)])

    def share(x):
        return [x] + [swap(x, slot) for slot in (1, 2, 3)]

    def over_z(x, columns):
        stride, kind = QUAD, x.dtype
        while True:
            got = [x] + [swap(x, way * stride) for way in (1, 2, 3)]
            stride *= 4
            if stride >= count:
                return got

            def add(*got):
                opened = [unpack(piece, traits, quarter, columns) for piece in got]
                sums = [by_pairs(list(column)) for column in zip(*(c for _, c in opened))]
                return (pack(by_pairs([wide for wide, _ in opened]), sums, kind),)

            if x.shape[0] == TILE:
                x = by_pairs(got)
            else:
                (x,) = fuse(add, *got)

    made = prepare(
        block_index, valid_counts, genotypes, coef_all, noise_coef, residual, noise_people, sigma2_old[None, :], prior_prec[None, :]
    )
    x_give, (noise_quarter, partial_res, kept, given, sent, noise_var, ridge, mask) = made[:QUAD], made[QUAD:]
    lines = kept.shape[0]
    back = swap(sent, 1)
    given = given + back[lines:]
    given, x_give = lax.optimization_barrier((given, x_give))
    far = swap(given, 2)
    kept = kept + back[:lines] + far
    x = [x_give[0]] + [swap(x_give[slot], slot) for slot in (1, 2, 3)]
    got = over_z(kept, 0)

    steps, betas, lows = [], [], []
    for number in range(ITERS):
        if number == 0:
            sent, search, low = fuse(first_search, *got, noise_quarter, noise_var, ridge, *x)
        else:
            sent, search, low, before, step = fuse(
                next_search, *got, search, direction, image, before, norm, length, noise_var, ridge, *x
            )
            steps.append(step)
        lows.append(low)
        (sent,) = fuse(functools.partial(over_core, IMAGE_KIND[number], 3 if number else 2, traits, rows), sent, swap(sent, 1))
        back = swap(sent, 2)
        if number == ITERS - 1:
            sent, image, norm, length, beta = fuse(last_sums, sent, back, mask, low, direction, image, norm, length, before)
            betas.append(beta)
            break
        state = (direction, image, norm, length) if number else ()
        sent, image, direction, norm, length, beta = fuse(
            functools.partial(people_part, PEOPLE_KIND[number], number == 0), sent, back, mask, low, *state, *x
        )
        if number:
            betas.append(beta)
        got = over_z(sent, 1)
        if number == 0:
            before = share(partial_res)
            got, before = lax.optimization_barrier((got, before))
            before = jnp.concatenate(before, axis=1)
        if number == ITERS - 2:
            early = share(jnp.concatenate(lows, axis=0))
            got, early = lax.optimization_barrier((got, early))

    late = share(low)
    got = over_z(sent, 4)
    coef_new, residual_new, sigma2_new = finish(
        block_index,
        valid_counts,
        got,
        norm,
        length,
        noise_var,
        ridge,
        gamma_draw[None, :],
        before,
        image,
        steps,
        betas,
        early,
        late,
        coef_all,
    )
    return (coef_new, residual_new, sigma2_new.reshape(-1))


def solution(mesh):
    return jax.shard_map(
        functools.partial(per_device, mesh.shape["ppl"]),
        mesh=mesh,
        in_specs=(
            P(("trait", "ppl"), None),
            P("trait", "ppl"),
            P("trait", "ppl"),
            P("trait", None),
            P("trait", None),
            P("trait"),
            P("trait"),
            P("trait"),
            P("trait"),
            P("trait"),
        ),
        out_specs=(P("trait", None), P("trait", "ppl"), P("trait")),
        check_vma=False,
    )
```

```python
import functools

import jax
import jax.numpy as jnp
from jax import lax
from jax.experimental import pallas as pl
from jax.experimental.pallas import tpu as pltpu
from jax.sharding import PartitionSpec as P


ITERS = 4
PRIOR_DOF = 4.0
PRIOR_SCALE = 0.5
LANES = 128
TILE = 8
QUAD = 4
F32, BF16 = jnp.float32, jnp.bfloat16
PEOPLE_KIND = (BF16, BF16, BF16)
IMAGE_KIND = (F32, BF16, BF16, BF16)
VMEM = pl.BlockSpec(memory_space=pltpu.VMEM)
SMEM = pl.BlockSpec(memory_space=pltpu.SMEM)
HBM = pl.BlockSpec(memory_space=pltpu.HBM)
PARAMS = pltpu.CompilerParams(vmem_limit_bytes=12 << 20)


def dot(a, b):
    return lax.dot_general(a, b, (((1,), (0,)), ((), ())), preferred_element_type=F32)


def dot_t(a, b):
    return lax.dot_general(a, b, (((1,), (1,)), ((), ())), preferred_element_type=F32)


def row_sum(values):
    return jnp.sum(values, axis=1, keepdims=True)


def by_pairs(terms):
    return (terms[0] + terms[1]) + (terms[2] + terms[3])


def diagonal(shape):
    return lax.broadcasted_iota(jnp.int32, shape, 0) == lax.broadcasted_iota(jnp.int32, shape, 1)


def to_row(column):
    same = diagonal((column.shape[0], LANES))
    return jnp.sum(jnp.where(same, column, 0.0), axis=0, keepdims=True)


def to_column(row, traits):
    same = diagonal((traits, row.shape[1]))
    return jnp.sum(jnp.where(same, row, 0.0), axis=1, keepdims=True)


def parts_of(value, kind):
    if kind == F32:
        return [value]
    first = value.astype(BF16)
    rest = value - first.astype(F32)
    second = rest.astype(BF16)
    return [first.astype(F32), second.astype(F32), rest - second.astype(F32)]


def pack(wide, columns, kind):
    _, width = wide.shape
    blocks = [wide[:, at : at + LANES].astype(kind) for at in range(0, width, LANES)]
    rows = [part for column in columns for part in parts_of(to_row(column), kind)]
    if rows:
        pad = -len(rows) % TILE
        rows.append(jnp.zeros((pad, LANES), F32))
        blocks.append(jnp.concatenate(rows, axis=0).astype(kind))
    return jnp.concatenate(blocks, axis=0)


def unpack(packed, traits, width, count=0):
    lines = traits * width // LANES
    wide = jnp.concatenate([packed[at : at + traits].astype(F32) for at in range(0, lines, traits)], axis=1)
    per = 1 if packed.dtype == F32 else 3
    rows = packed[lines:].astype(F32)
    columns = []
    for index in range(count):
        mine = [rows[index * per + k : index * per + k + 1] for k in range(per)]
        row = mine[0] if per == 1 else (mine[2] + mine[1]) + mine[0]
        columns.append(to_column(row, traits))
    return wide, columns


def fuse(fn, *args):
    shapes = jax.eval_shape(fn, *args)

    def kernel(*refs):
        ins, outs = refs[: len(args)], refs[len(args) :]
        for out, value in zip(outs, fn(*(ref[...] for ref in ins))):
            out[...] = value

    return pl.pallas_call(kernel, out_shape=shapes, compiler_params=PARAMS, in_specs=[VMEM] * len(args), out_specs=[VMEM] * len(shapes))(*args)


def place_in_quad():
    return lax.axis_index("ppl") & (QUAD - 1)


def prepare(block_index, valid_counts, genotypes, coef_all, noise_coef, residual, noise_people, sigma2_old, prior_prec):
    rows, width = genotypes.shape
    traits = residual.shape[0]
    quarter = width // QUAD

    def kernel(block_ref, valid_ref, geno_ref, coef_ref, noise_ref, *refs):
        wanted, x_refs, refs = refs[:4], refs[4 : 4 + QUAD], refs[4 + QUAD :]
        noise_out, partial_ref, kept_ref, given_ref, cross_ref, var_ref, ridge_ref, mask_ref, old_ref, *landed, sems = refs
        me = lax.axis_index("ppl")
        own = place_in_quad()
        copies = []
        for slot in range(QUAD):
            start = pl.multiple_of((own ^ slot) * quarter, LANES)
            first = pl.multiple_of(block_ref[0] * width + start, LANES)
            pair = (
                pltpu.make_async_copy(coef_ref.at[:, pl.ds(first, quarter)], old_ref.at[slot], sems.at[2 * slot]),
                pltpu.make_async_copy(geno_ref.at[:, pl.ds(start, quarter)], x_refs[slot], sems.at[2 * slot + 1]),
            )
            for copy in pair:
                copy.start()
            copies.append(pair)
        start = pl.multiple_of(own * quarter, LANES)
        last = pltpu.make_async_copy(noise_ref.at[:, pl.ds(start, quarter)], noise_out, sems.at[2 * QUAD])
        small = [pltpu.make_async_copy(a, b, sems.at[2 * QUAD + 1 + k]) for k, (a, b) in enumerate(zip(wanted, landed))]
        for copy in (*small, last):
            copy.start()
        for copy in small:
            copy.wait()
        res_ref, people_ref, sigma_ref, prior_ref = landed
        noise_var = to_column(sigma_ref[...], traits)
        var_ref[...] = noise_var
        ridge_ref[...] = to_column(prior_ref[...], traits)
        fitted = jnp.zeros((traits, rows), F32)
        for slot in range(QUAD):
            for copy in copies[slot]:
                copy.wait()
            fitted += dot_t(old_ref[slot].astype(BF16), x_refs[slot][...])
        slots = lax.broadcasted_iota(jnp.int32, (1, rows), 1)
        for slot in range(QUAD):
            mask_ref[:, slot * rows : (slot + 1) * rows] = (slots < valid_ref[me ^ slot]).astype(F32)
        present = (slots < valid_ref[me]).astype(F32)
        partial = present * (res_ref[...] + fitted)
        partial_ref[...] = partial
        target = (present * (partial + jnp.sqrt(noise_var) * people_ref[...])).astype(BF16)
        lines = traits * quarter // LANES
        cross_ref[:lines] = pack(dot(target, x_refs[1][...]), (), F32)
        cross_ref[lines:] = pack(dot(target, x_refs[3][...]), (), F32)
        given_ref[...] = pack(dot(target, x_refs[2][...]), (), F32)
        kept_ref[...] = pack(dot(target, x_refs[0][...]), (), F32)
        last.wait()

    lines = traits * quarter // LANES
    shape = jax.ShapeDtypeStruct
    out_shape = [shape((rows, quarter), BF16)] * QUAD + [
        shape((traits, quarter), F32),
        shape((traits, rows), F32),
        shape((lines, LANES), F32),
        shape((lines, LANES), F32),
        shape((2 * lines, LANES), F32),
        shape((traits, 1), F32),
        shape((traits, 1), F32),
        shape((1, QUAD * rows), F32),
    ]
    return pl.pallas_call(
        kernel,
        compiler_params=PARAMS,
        out_shape=out_shape,
        in_specs=[SMEM, SMEM] + [HBM] * 7,
        out_specs=[VMEM] * len(out_shape),
        scratch_shapes=[
            pltpu.VMEM((QUAD, traits, quarter), F32),
            *(pltpu.VMEM(array.shape, F32) for array in (residual, noise_people, sigma2_old, prior_prec)),
            pltpu.SemaphoreType.DMA((2 * QUAD + 5,)),
        ],
    )(block_index, valid_counts, genotypes, coef_all, noise_coef, residual, noise_people, sigma2_old, prior_prec)


def image_part(search, direction, x):
    low = search.astype(BF16)
    wide = low.astype(F32)
    sums = [row_sum(search * search), row_sum(wide * wide)]
    if direction is not None:
        sums.append(row_sum(wide * direction))
    image = jnp.concatenate([dot_t(low, block) for block in x], axis=1)
    return pack(image, sums, F32), search, low


def first_search(got0, got1, got2, got3, noise_coef, noise_var, ridge, *x):
    traits, quarter = noise_coef.shape
    total, _ = unpack((got0 + got1) + (got2 + got3), traits, quarter)
    return image_part(total / noise_var + jnp.sqrt(ridge) * noise_coef, None, x)


def next_search(got0, got1, got2, got3, search, direction, image, before, norm, length, noise_var, ridge, *x):
    traits, quarter = search.shape
    opened = [unpack(got, traits, quarter, 1) for got in (got0, got1, got2, got3)]
    total = by_pairs([wide for wide, _ in opened])
    energy = by_pairs([columns[0] for _, columns in opened])
    step = norm / (energy / noise_var + ridge * length)
    search = search - step * (total / noise_var + ridge * direction)
    return *image_part(search, direction, x), before - step * image, step


def cross(packed, way, traits, rows):
    lines = traits * rows // LANES
    blocks = [packed[(slot ^ way) * lines : ((slot ^ way) + 1) * lines] for slot in range(QUAD)]
    return jnp.concatenate(blocks + [packed[QUAD * lines :]], axis=0)


def over_core(kind, count, traits, rows, sent, back):
    total = sent + cross(back, 1, traits, rows)
    if kind == F32:
        return (total,)
    wide, columns = unpack(total, traits, QUAD * rows, count)
    return (pack(wide, columns, kind),)


def new_image(count, sent, back, mask, low, direction, image, norm_old, length):
    traits = low.shape[0]
    rows = mask.shape[1] // QUAD
    wide, columns = unpack(sent, traits, QUAD * rows, count)
    far, far_columns = unpack(cross(back, 2, traits, rows), traits, QUAD * rows, count)
    columns = [a + b for a, b in zip(columns, far_columns)]
    fresh = mask * (wide + far)
    norm, low_low = columns[:2]
    wide = low.astype(F32)
    if direction is None:
        return fresh, wide, norm, low_low, jnp.zeros_like(norm)
    beta = norm / norm_old
    length = low_low + beta * (2.0 * columns[2] + beta * length)
    return fresh + beta * image, wide + beta * direction, norm, length, beta


def slots_of(wide, rows):
    return [wide[:, slot * rows : (slot + 1) * rows] for slot in range(QUAD)]


def people_part(kind, first, sent, back, mask, low, *rest):
    if first:
        state, x = new_image(2, sent, back, mask, low, None, None, None, None), rest
    else:
        state, x = new_image(3, sent, back, mask, low, *rest[:4]), rest[4:]
    rounded = state[0].astype(BF16)
    rows = mask.shape[1] // QUAD
    energy = by_pairs([row_sum(part) for part in slots_of(state[0] * rounded.astype(F32), rows)])
    total, at = 0.0, 0
    for block in x:
        total += dot(rounded[:, at : at + block.shape[0]], block)
        at += block.shape[0]
    return pack(total, [energy], kind), *state


def last_sums(sent, back, mask, low, direction, image, norm_old, length, before):
    image, _, norm, length, beta = new_image(3, sent, back, mask, low, direction, image, norm_old, length)
    rows = mask.shape[1] // QUAD
    products = (image * image.astype(BF16).astype(F32), before * before, before * image, image * image)
    sums = [to_row(by_pairs([row_sum(part) for part in slots_of(product, rows)])) for product in products]
    packed = jnp.concatenate(sums + [jnp.zeros((TILE - len(sums), LANES), F32)], axis=0)
    return packed, image[:, :rows], norm, length, beta


def finish(block_index, valid_counts, got, norm, length, noise_var, ridge, gamma, before, image, steps, betas, early, late, coef_all):
    traits, quarter = late[0].shape
    rows = image.shape[1]
    width = QUAD * quarter
    blocks = coef_all.shape[1] // width
    kept = ITERS - 1
    args = [*got, norm, length, noise_var, ridge, gamma, before, image, *steps, *betas, *early, *late]
    split = [len(got), 7, kept, kept, kept * QUAD, QUAD]

    def kernel(block_ref, valid_ref, *refs):
        groups, at = [], 0
        for size in split:
            groups.append(refs[at : at + size])
            at += size
        coef_ref, out_ref, res_ref, sigma_ref, scratch, sems = refs[at:]
        block, own = block_ref[0], place_in_quad()

        def hold(index):
            span = pl.ds(index * width, width)
            return pltpu.make_async_copy(coef_ref.at[:, span], out_ref.at[:, span], sems.at[index])

        def give(slot):
            start = pl.multiple_of(block * width + (own ^ slot) * quarter, LANES)
            return pltpu.make_async_copy(scratch.at[slot], out_ref.at[:, pl.ds(start, quarter)], sems.at[blocks + slot])

        for index in range(blocks):
            pl.when(block != index)(lambda index=index: hold(index).start())
        got, (norm, length, noise_var, ridge, gamma, before, image), steps, betas, early, late = groups
        total = by_pairs([ref[...] for ref in got]) if len(got) == QUAD else got[0][...]
        energy, squares, mixed, energy_full = (to_column(total[k : k + 1], traits) for k in range(4))
        step = norm[...] / (energy / noise_var[...] + ridge[...] * length[...])
        scale, mix = [], []
        for number in range(ITERS):
            mix = [betas[number - 1][...] * m for m in mix] + [jnp.ones_like(step)]
            now = steps[number][...] if number < kept else step
            scale = [s + now * m for s, m in zip(scale + [jnp.zeros_like(step)], mix)]
        for slot in range(QUAD):
            value = scale[kept] * late[slot][...].astype(F32)
            for k in range(kept):
                value += scale[k] * early[k * QUAD + slot][...].astype(F32)
            scratch[slot] = value
            give(slot).start()
        res_ref[...] = before[:, :rows] - step * image[...]
        squares = squares - step * (2.0 * mixed - step * energy_full)
        present = sum(valid_ref[k] for k in range(valid_counts.shape[0])).astype(F32)
        row = to_row(squares + PRIOR_DOF * PRIOR_SCALE)[:, :traits]
        sigma_ref[...] = row / ((present + PRIOR_DOF) * gamma[...])
        for slot in range(QUAD):
            give(slot).wait()
        for index in range(blocks):
            pl.when(block != index)(lambda index=index: hold(index).wait())

    shape = jax.ShapeDtypeStruct
    return pl.pallas_call(
        kernel,
        compiler_params=PARAMS,
        out_shape=[shape(coef_all.shape, F32), shape((traits, rows), F32), shape((1, traits), F32)],
        in_specs=[SMEM, SMEM] + [VMEM] * (len(args) + 1),
        out_specs=[HBM, VMEM, VMEM],
        scratch_shapes=[pltpu.VMEM((QUAD, traits, quarter), F32), pltpu.SemaphoreType.DMA((blocks + QUAD,))],
    )(block_index, valid_counts, *args, coef_all)


def per_device(
    count,
    genotypes,
    residual,
    noise_people,
    noise_coef,
    coef_all,
    block_index,
    prior_prec,
    sigma2_old,
    gamma_draw,
    valid_counts,
):
    rows, width = genotypes.shape
    traits = residual.shape[0]
    quarter = width // QUAD

    def swap(x, distance):
        return lax.ppermute(x, "ppl", [(i, i ^ distance) for i in range(count)])

    def share(x):
        return [x] + [swap(x, slot) for slot in (1, 2, 3)]

    def over_z(x, columns):
        stride, kind = QUAD, x.dtype
        while True:
            got = [x] + [swap(x, way * stride) for way in (1, 2, 3)]
            stride *= 4
            if stride >= count:
                return got

            def add(*got):
                opened = [unpack(piece, traits, quarter, columns) for piece in got]
                sums = [by_pairs(list(column)) for column in zip(*(c for _, c in opened))]
                return (pack(by_pairs([wide for wide, _ in opened]), sums, kind),)

            if x.shape[0] == TILE:
                x = by_pairs(got)
            else:
                (x,) = fuse(add, *got)

    ahead = rows // 2
    corner = (0, (place_in_quad() ^ 2) * (width // QUAD))
    head = swap(lax.dynamic_slice(genotypes, corner, (ahead, width // QUAD)), 2)
    columns = sigma2_old[None, :], prior_prec[None, :]
    made = prepare(block_index, valid_counts, genotypes, coef_all, noise_coef, residual, noise_people, *columns)
    x_give, (noise_quarter, partial_res, kept, given, sent, noise_var, ridge, mask) = made[:QUAD], made[QUAD:]
    lines = kept.shape[0]
    back = swap(sent, 1)
    given = given + back[lines:]
    x_give = [x_give[0], x_give[1], x_give[2][ahead:], x_give[3]]
    given, x_give = lax.optimization_barrier((given, x_give))
    far = swap(given, 2)
    kept = kept + back[:lines] + far
    near, across, far_x = (swap(x_give[slot], slot) for slot in (1, 2, 3))
    x = [x_give[0], near, head, across, far_x]
    got = over_z(kept, 0)

    steps, betas, early = [], [], []
    for number in range(ITERS):
        if number == 0:
            sent, search, low = fuse(first_search, *got, noise_quarter, noise_var, ridge, *x)
        else:
            sent, search, low, before, step = fuse(
                next_search, *got, search, direction, image, before, norm, length, noise_var, ridge, *x
            )
            steps.append(step)
        (sent,) = fuse(functools.partial(over_core, IMAGE_KIND[number], 3 if number else 2, traits, rows), sent, swap(sent, 1))
        back = swap(sent, 2)
        if number == ITERS - 1:
            sent, image, norm, length, beta = fuse(last_sums, sent, back, mask, low, direction, image, norm, length, before)
            betas.append(beta)
            break
        state = (direction, image, norm, length) if number else ()
        sent, image, direction, norm, length, beta = fuse(
            functools.partial(people_part, PEOPLE_KIND[number], number == 0), sent, back, mask, low, *state, *x
        )
        if number:
            betas.append(beta)
        got = over_z(sent, 1)
        spread = share(low) + (share(partial_res) if number == 0 else [])
        got, spread = lax.optimization_barrier((got, spread))
        if number == 0:
            before = jnp.concatenate(spread[QUAD:], axis=1)
        early += spread[:QUAD]

    late = share(low)
    got = over_z(sent, 4)
    coef_new, residual_new, sigma2_new = finish(
        block_index,
        valid_counts,
        got,
        norm,
        length,
        noise_var,
        ridge,
        gamma_draw[None, :],
        before,
        image,
        steps,
        betas,
        early,
        late,
        coef_all,
    )
    return (coef_new, residual_new, sigma2_new.reshape(-1))


def solution(mesh):
    return jax.shard_map(
        functools.partial(per_device, mesh.shape["ppl"]),
        mesh=mesh,
        in_specs=(
            P(("trait", "ppl"), None),
            P("trait", "ppl"),
            P("trait", "ppl"),
            P("trait", None),
            P("trait", None),
            P("trait"),
            P("trait"),
            P("trait"),
            P("trait"),
            P("trait"),
        ),
        out_specs=(P("trait", None), P("trait", "ppl"), P("trait")),
        check_vma=False,
    )
```

```python
import functools

import jax
import jax.numpy as jnp
from jax import lax
from jax.experimental import pallas as pl
from jax.experimental.pallas import tpu as pltpu
from jax.sharding import PartitionSpec as P


ITERS = 4
PRIOR_DOF = 4.0
PRIOR_SCALE = 0.5
LANES = 128
TILE = 8
QUAD = 4
F32, BF16 = jnp.float32, jnp.bfloat16
PEOPLE_KIND = (BF16, BF16, BF16)
IMAGE_KIND = (F32, BF16, BF16, BF16)
VMEM = pl.BlockSpec(memory_space=pltpu.VMEM)
SMEM = pl.BlockSpec(memory_space=pltpu.SMEM)
HBM = pl.BlockSpec(memory_space=pltpu.HBM)
PARAMS = pltpu.CompilerParams(vmem_limit_bytes=12 << 20)


def dot(a, b):
    return lax.dot_general(a, b, (((1,), (0,)), ((), ())), preferred_element_type=F32)


def dot_t(a, b):
    return lax.dot_general(a, b, (((1,), (1,)), ((), ())), preferred_element_type=F32)


def row_sum(values):
    return jnp.sum(values, axis=1, keepdims=True)


def by_pairs(terms):
    return (terms[0] + terms[1]) + (terms[2] + terms[3])


def diagonal(shape):
    return lax.broadcasted_iota(jnp.int32, shape, 0) == lax.broadcasted_iota(jnp.int32, shape, 1)


def to_row(column):
    same = diagonal((column.shape[0], LANES))
    return jnp.sum(jnp.where(same, column, 0.0), axis=0, keepdims=True)


def to_column(row, traits):
    same = diagonal((traits, row.shape[1]))
    return jnp.sum(jnp.where(same, row, 0.0), axis=1, keepdims=True)


def parts_of(value, kind):
    if kind == F32:
        return [value]
    first = value.astype(BF16)
    rest = value - first.astype(F32)
    second = rest.astype(BF16)
    return [first.astype(F32), second.astype(F32), rest - second.astype(F32)]


def pack(wide, columns, kind):
    _, width = wide.shape
    blocks = [wide[:, at : at + LANES].astype(kind) for at in range(0, width, LANES)]
    rows = [part for column in columns for part in parts_of(to_row(column), kind)]
    if rows:
        pad = -len(rows) % TILE
        rows.append(jnp.zeros((pad, LANES), F32))
        blocks.append(jnp.concatenate(rows, axis=0).astype(kind))
    return jnp.concatenate(blocks, axis=0)


def unpack(packed, traits, width, count=0):
    lines = traits * width // LANES
    wide = jnp.concatenate([packed[at : at + traits].astype(F32) for at in range(0, lines, traits)], axis=1)
    per = 1 if packed.dtype == F32 else 3
    rows = packed[lines:].astype(F32)
    columns = []
    for index in range(count):
        mine = [rows[index * per + k : index * per + k + 1] for k in range(per)]
        row = mine[0] if per == 1 else (mine[2] + mine[1]) + mine[0]
        columns.append(to_column(row, traits))
    return wide, columns


def fuse(fn, *args):
    shapes = jax.eval_shape(fn, *args)

    def kernel(*refs):
        ins, outs = refs[: len(args)], refs[len(args) :]
        for out, value in zip(outs, fn(*(ref[...] for ref in ins))):
            out[...] = value

    return pl.pallas_call(kernel, out_shape=shapes, compiler_params=PARAMS, in_specs=[VMEM] * len(args), out_specs=[VMEM] * len(shapes))(*args)


def place_in_quad():
    return lax.axis_index("ppl") & (QUAD - 1)


def prepare(block_index, valid_counts, genotypes, coef_all, noise_coef, residual, noise_people, sigma2_old, prior_prec):
    operands = genotypes, coef_all, noise_coef, valid_counts, residual, noise_people, sigma2_old, prior_prec
    rows, width = genotypes.shape
    traits = residual.shape[0]
    quarter = width // QUAD

    def kernel(block_ref, geno_ref, coef_ref, noise_ref, *refs):
        wanted, x_refs, (noise_out, partial_ref, *refs) = refs[:5], refs[5 : 5 + QUAD], refs[5 + QUAD :]
        kept_ref, given_ref, cross_ref, var_ref, ridge_ref, mask_ref, present_ref, old_ref, *landed, sems = refs
        me = lax.axis_index("ppl")
        own = place_in_quad()
        small = [pltpu.make_async_copy(a, b, sems.at[2 * QUAD + 1 + k]) for k, (a, b) in enumerate(zip(wanted, landed))]
        for copy in small:
            copy.start()
        valid_ref, res_ref, people_ref, sigma_ref, prior_ref = landed
        copies = []
        for slot in range(QUAD):
            span = pl.ds(pl.multiple_of((own ^ slot) * quarter, LANES), quarter)
            first = pl.multiple_of(block_ref[0] * width + (own ^ slot) * quarter, LANES)
            pair = (
                pltpu.make_async_copy(coef_ref.at[:, pl.ds(first, quarter)], old_ref.at[slot], sems.at[QUAD + slot]),
                pltpu.make_async_copy(geno_ref.at[:, span], x_refs[slot], sems.at[slot]),
            )
            for copy in pair:
                copy.start()
            copies.append(pair)
        span = pl.ds(pl.multiple_of(own * quarter, LANES), quarter)
        last = pltpu.make_async_copy(noise_ref.at[:, span], noise_out, sems.at[2 * QUAD])
        last.start()
        for copy in small:
            copy.wait()
        present = sum(valid_ref[k] for k in range(valid_counts.shape[0]))
        present_ref[...] = jnp.full((1, traits), present, jnp.int32).astype(F32)
        noise_var = to_column(sigma_ref[...], traits)
        var_ref[...] = noise_var
        ridge_ref[...] = to_column(prior_ref[...], traits)
        fitted = jnp.zeros((traits, rows), F32)
        for slot in range(QUAD):
            for copy in copies[slot]:
                copy.wait()
            fitted += dot_t(old_ref[slot].astype(BF16), x_refs[slot][...])
        slots = lax.broadcasted_iota(jnp.int32, (1, rows), 1)
        for slot in range(QUAD):
            mask_ref[:, slot * rows : (slot + 1) * rows] = (slots < valid_ref[me ^ slot]).astype(F32)
        present = (slots < valid_ref[me]).astype(F32)
        partial = present * (res_ref[...] + fitted)
        partial_ref[...] = partial
        target = (present * (partial + jnp.sqrt(noise_var) * people_ref[...])).astype(BF16)
        lines = traits * quarter // LANES
        cross_ref[:lines] = pack(dot(target, x_refs[1][...]), (), F32)
        cross_ref[lines:] = pack(dot(target, x_refs[3][...]), (), F32)
        given_ref[...] = pack(dot(target, x_refs[2][...]), (), F32)
        kept_ref[...] = pack(dot(target, x_refs[0][...]), (), F32)
        last.wait()

    lines = traits * quarter // LANES
    shape = jax.ShapeDtypeStruct
    out_shape = [shape((rows, quarter), BF16)] * QUAD + [
        shape((traits, quarter), F32),
        shape((traits, rows), F32),
        shape((lines, LANES), F32),
        shape((lines, LANES), F32),
        shape((2 * lines, LANES), F32),
        shape((traits, 1), F32),
        shape((traits, 1), F32),
        shape((1, QUAD * rows), F32),
        shape((1, traits), F32),
    ]
    return pl.pallas_call(
        kernel,
        compiler_params=PARAMS,
        out_shape=out_shape,
        in_specs=[SMEM] + [HBM] * 8,
        out_specs=[VMEM] * len(out_shape),
        scratch_shapes=[
            pltpu.VMEM((QUAD, traits, quarter), F32),
            pltpu.SMEM(valid_counts.shape, jnp.int32),
            *(pltpu.VMEM(array.shape, F32) for array in (residual, noise_people, sigma2_old, prior_prec)),
            pltpu.SemaphoreType.DMA((2 * QUAD + 6,)),
        ],
    )(block_index, *(pltpu.with_memory_space_constraint(array, pltpu.HBM) for array in operands))


def image_part(search, direction, x):
    low = search.astype(BF16)
    wide = low.astype(F32)
    sums = [row_sum(search * search), row_sum(wide * wide)]
    if direction is not None:
        sums.append(row_sum(wide * direction))
    image = jnp.concatenate([dot_t(low, block) for block in x], axis=1)
    return pack(image, sums, F32), search, low


def first_search(got0, got1, got2, got3, noise_coef, noise_var, ridge, *x):
    traits, quarter = noise_coef.shape
    total, _ = unpack((got0 + got1) + (got2 + got3), traits, quarter)
    return image_part(total / noise_var + jnp.sqrt(ridge) * noise_coef, None, x)


def next_search(first, got0, got1, got2, got3, search, direction, image, norm, length, noise_var, ridge, *x):
    fitted, x = (0.0, x) if first else (x[0], x[1:])
    traits, quarter = search.shape
    opened = [unpack(got, traits, quarter, 1) for got in (got0, got1, got2, got3)]
    total = by_pairs([wide for wide, _ in opened])
    energy = by_pairs([columns[0] for _, columns in opened])
    step = norm / (energy / noise_var + ridge * length)
    search = search - step * (total / noise_var + ridge * direction)
    return *image_part(search, direction, x), fitted + step * image, step


def cross(packed, way, traits, rows):
    lines = traits * rows // LANES
    blocks = [packed[(slot ^ way) * lines : ((slot ^ way) + 1) * lines] for slot in range(QUAD)]
    return jnp.concatenate(blocks + [packed[QUAD * lines :]], axis=0)


def over_core(kind, count, traits, rows, sent, back):
    total = sent + cross(back, 1, traits, rows)
    if kind == F32:
        return (total,)
    wide, columns = unpack(total, traits, QUAD * rows, count)
    return (pack(wide, columns, kind),)


def new_image(count, sent, back, mask, low, direction, image, norm_old, length):
    traits = low.shape[0]
    rows = mask.shape[1] // QUAD
    wide, columns = unpack(sent, traits, QUAD * rows, count)
    far, far_columns = unpack(cross(back, 2, traits, rows), traits, QUAD * rows, count)
    columns = [a + b for a, b in zip(columns, far_columns)]
    fresh = mask * (wide + far)
    norm, low_low = columns[:2]
    wide = low.astype(F32)
    if direction is None:
        return fresh, wide, norm, low_low, jnp.zeros_like(norm)
    beta = norm / norm_old
    length = low_low + beta * (2.0 * columns[2] + beta * length)
    return fresh + beta * image, wide + beta * direction, norm, length, beta


def slots_of(wide, rows):
    return [wide[:, slot * rows : (slot + 1) * rows] for slot in range(QUAD)]


def people_part(kind, first, sent, back, mask, low, *rest):
    if first:
        state, x = new_image(2, sent, back, mask, low, None, None, None, None), rest
    else:
        state, x = new_image(3, sent, back, mask, low, *rest[:4]), rest[4:]
    rounded = state[0].astype(BF16)
    rows = mask.shape[1] // QUAD
    energy = by_pairs([row_sum(part) for part in slots_of(state[0] * rounded.astype(F32), rows)])
    total, at = 0.0, 0
    for block in x:
        total += dot(rounded[:, at : at + block.shape[0]], block)
        at += block.shape[0]
    return pack(total, [energy], kind), *state


def last_sums(sent, back, mask, low, direction, image, norm_old, length, fitted, *partial):
    before = jnp.concatenate(partial, axis=1) - fitted
    image, _, norm, length, beta = new_image(3, sent, back, mask, low, direction, image, norm_old, length)
    rows = mask.shape[1] // QUAD
    products = (image * image.astype(BF16).astype(F32), before * before, before * image, image * image)
    sums = [to_row(by_pairs([row_sum(part) for part in slots_of(product, rows)])) for product in products]
    packed = jnp.concatenate(sums + [jnp.zeros((TILE - len(sums), LANES), F32)], axis=0)
    return packed, before[:, :rows], image[:, :rows], norm, length, beta


def finish(block_index, present, got, norm, length, noise_var, ridge, gamma, before, image, steps, betas, early, late, coef_all):
    traits, quarter = late[0].shape
    rows = image.shape[1]
    width = QUAD * quarter
    blocks = coef_all.shape[1] // width
    kept = ITERS - 1
    args = [*got, norm, length, noise_var, ridge, gamma, before, image, *steps, *betas, *early, *late]
    split = [len(got), 7, kept, kept, kept * QUAD, QUAD]

    def kernel(block_ref, present_ref, *refs):
        groups, at = [], 0
        for size in split:
            groups.append(refs[at : at + size])
            at += size
        coef_ref, out_ref, res_ref, sigma_ref, scratch, sems = refs[at:]
        block, own = block_ref[0], place_in_quad()

        def hold(index):
            span = pl.ds(index * width, width)
            return pltpu.make_async_copy(coef_ref.at[:, span], out_ref.at[:, span], sems.at[index])

        def give(slot):
            start = pl.multiple_of(block * width + (own ^ slot) * quarter, LANES)
            return pltpu.make_async_copy(scratch.at[slot], out_ref.at[:, pl.ds(start, quarter)], sems.at[blocks + slot])

        for index in range(blocks):
            pl.when(block != index)(lambda index=index: hold(index).start())
        got, (norm, length, noise_var, ridge, gamma, before, image), steps, betas, early, late = groups
        total = by_pairs([ref[...] for ref in got]) if len(got) == QUAD else got[0][...]
        energy, squares, mixed, energy_full = (to_column(total[k : k + 1], traits) for k in range(4))
        step = norm[...] / (energy / noise_var[...] + ridge[...] * length[...])
        scale, mix = [], []
        for number in range(ITERS):
            mix = [betas[number - 1][...] * m for m in mix] + [jnp.ones_like(step)]
            now = steps[number][...] if number < kept else step
            scale = [s + now * m for s, m in zip(scale + [jnp.zeros_like(step)], mix)]
        for slot in range(QUAD):
            value = scale[kept] * late[slot][...].astype(F32)
            for k in range(kept):
                value += scale[k] * early[k * QUAD + slot][...].astype(F32)
            scratch[slot] = value
            give(slot).start()
        res_ref[...] = before[...] - step * image[...]
        squares = squares - step * (2.0 * mixed - step * energy_full)
        row = to_row(squares + PRIOR_DOF * PRIOR_SCALE)[:, :traits]
        sigma_ref[...] = row / ((present_ref[...] + PRIOR_DOF) * gamma[...])
        for slot in range(QUAD):
            give(slot).wait()
        for index in range(blocks):
            pl.when(block != index)(lambda index=index: hold(index).wait())

    shape = jax.ShapeDtypeStruct
    return pl.pallas_call(
        kernel,
        compiler_params=PARAMS,
        out_shape=[shape(coef_all.shape, F32), shape((traits, rows), F32), shape((1, traits), F32)],
        in_specs=[SMEM] + [VMEM] * (len(args) + 2),
        out_specs=[HBM, VMEM, VMEM],
        scratch_shapes=[pltpu.VMEM((QUAD, traits, quarter), F32), pltpu.SemaphoreType.DMA((blocks + QUAD,))],
    )(block_index, present, *args, coef_all)


def per_device(
    count,
    genotypes,
    residual,
    noise_people,
    noise_coef,
    coef_all,
    block_index,
    prior_prec,
    sigma2_old,
    gamma_draw,
    valid_counts,
):
    rows, width = genotypes.shape
    traits = residual.shape[0]
    quarter = width // QUAD

    def swap(x, distance):
        return lax.ppermute(x, "ppl", [(i, i ^ distance) for i in range(count)])

    def share(x):
        return [x] + [swap(x, slot) for slot in (1, 2, 3)]

    def over_z(x, columns):
        stride, kind = QUAD, x.dtype
        while True:
            got = [x] + [swap(x, way * stride) for way in (1, 2, 3)]
            stride *= 4
            if stride >= count:
                return got

            def add(*got):
                opened = [unpack(piece, traits, quarter, columns) for piece in got]
                sums = [by_pairs(list(column)) for column in zip(*(c for _, c in opened))]
                return (pack(by_pairs([wide for wide, _ in opened]), sums, kind),)

            if x.shape[0] == TILE:
                x = by_pairs(got)
            else:
                (x,) = fuse(add, *got)

    ahead = rows // 2
    corner = (0, (place_in_quad() ^ 2) * (width // QUAD))
    head = swap(lax.dynamic_slice(genotypes, corner, (ahead, width // QUAD)), 2)
    columns = sigma2_old[None, :], prior_prec[None, :]
    made = prepare(block_index, valid_counts, genotypes, coef_all, noise_coef, residual, noise_people, *columns)
    x_give, (noise_quarter, partial_res, kept, given, sent, noise_var, ridge, mask, present) = made[:QUAD], made[QUAD:]
    lines = kept.shape[0]
    back = swap(sent, 1)
    given = given + back[lines:]
    x_give = [x_give[0], x_give[1], x_give[2][ahead:], x_give[3]]
    given, x_give = lax.optimization_barrier((given, x_give))
    far = swap(given, 2)
    kept = kept + back[:lines] + far
    near, across, far_x = (swap(x_give[slot], slot) for slot in (1, 2, 3))
    x = [x_give[0], near, head, across, far_x]
    got = over_z(kept, 0)
    partial = share(partial_res)

    steps, betas, early = [], [], []
    for number in range(ITERS):
        if number == 0:
            sent, search, low = fuse(first_search, *got, noise_quarter, noise_var, ridge, *x)
        else:
            held = () if number == 1 else (fitted,)
            sent, search, low, fitted, step = fuse(
                functools.partial(next_search, number == 1), *got, search, direction, image, norm, length, noise_var, ridge, *held, *x
            )
            steps.append(step)
        (sent,) = fuse(functools.partial(over_core, IMAGE_KIND[number], 3 if number else 2, traits, rows), sent, swap(sent, 1))
        back = swap(sent, 2)
        if number == ITERS - 1:
            sent, before, image, norm, length, beta = fuse(
                last_sums, sent, back, mask, low, direction, image, norm, length, fitted, *partial
            )
            betas.append(beta)
            break
        state = (direction, image, norm, length) if number else ()
        sent, image, direction, norm, length, beta = fuse(
            functools.partial(people_part, PEOPLE_KIND[number], number == 0), sent, back, mask, low, *state, *x
        )
        if number:
            betas.append(beta)
        got = over_z(sent, 1)
        early += share(low)

    late = share(low)
    got = over_z(sent, 4)
    coef_new, residual_new, sigma2_new = finish(
        block_index,
        present,
        got,
        norm,
        length,
        noise_var,
        ridge,
        gamma_draw[None, :],
        before,
        image,
        steps,
        betas,
        early,
        late,
        coef_all,
    )
    return (coef_new, residual_new, sigma2_new.reshape(-1))


def solution(mesh):
    return jax.shard_map(
        functools.partial(per_device, mesh.shape["ppl"]),
        mesh=mesh,
        in_specs=(
            P(("trait", "ppl"), None),
            P("trait", "ppl"),
            P("trait", "ppl"),
            P("trait", None),
            P("trait", None),
            P("trait"),
            P("trait"),
            P("trait"),
            P("trait"),
            P("trait"),
        ),
        out_specs=(P("trait", None), P("trait", "ppl"), P("trait")),
        check_vma=False,
    )
```

```python
import functools

import jax
import jax.numpy as jnp
from jax import lax
from jax.experimental import pallas as pl
from jax.experimental.pallas import tpu as pltpu
from jax.sharding import PartitionSpec as P


ITERS = 4
PRIOR_DOF = 4.0
PRIOR_SCALE = 0.5
LANES = 128
TILE = 8
QUAD = 4
F32, BF16 = jnp.float32, jnp.bfloat16
PEOPLE_KIND = (BF16, BF16, BF16)
IMAGE_KIND = (F32, BF16, BF16, BF16)
VMEM = pl.BlockSpec(memory_space=pltpu.VMEM)
SMEM = pl.BlockSpec(memory_space=pltpu.SMEM)
HBM = pl.BlockSpec(memory_space=pltpu.HBM)
PARAMS = pltpu.CompilerParams(vmem_limit_bytes=12 << 20)


def dot(a, b):
    return lax.dot_general(a, b, (((1,), (0,)), ((), ())), preferred_element_type=F32)


def dot_t(a, b):
    return lax.dot_general(a, b, (((1,), (1,)), ((), ())), preferred_element_type=F32)


def row_sum(values):
    return jnp.sum(values, axis=1, keepdims=True)


def by_pairs(terms):
    return (terms[0] + terms[1]) + (terms[2] + terms[3])


def diagonal(shape):
    return lax.broadcasted_iota(jnp.int32, shape, 0) == lax.broadcasted_iota(jnp.int32, shape, 1)


def to_row(column):
    same = diagonal((column.shape[0], LANES))
    return jnp.sum(jnp.where(same, column, 0.0), axis=0, keepdims=True)


def to_column(row, traits):
    same = diagonal((traits, row.shape[1]))
    return jnp.sum(jnp.where(same, row, 0.0), axis=1, keepdims=True)


def parts_of(value, kind):
    if kind == F32:
        return [value]
    first = value.astype(BF16)
    rest = value - first.astype(F32)
    second = rest.astype(BF16)
    return [first.astype(F32), second.astype(F32), rest - second.astype(F32)]


def pack(wide, columns, kind):
    _, width = wide.shape
    blocks = [wide[:, at : at + LANES].astype(kind) for at in range(0, width, LANES)]
    rows = [part for column in columns for part in parts_of(to_row(column), kind)]
    if rows:
        pad = -len(rows) % TILE
        rows.append(jnp.zeros((pad, LANES), F32))
        blocks.append(jnp.concatenate(rows, axis=0).astype(kind))
    return jnp.concatenate(blocks, axis=0)


def unpack(packed, traits, width, count=0):
    lines = traits * width // LANES
    wide = jnp.concatenate([packed[at : at + traits].astype(F32) for at in range(0, lines, traits)], axis=1)
    per = 1 if packed.dtype == F32 else 3
    rows = packed[lines:].astype(F32)
    columns = []
    for index in range(count):
        mine = [rows[index * per + k : index * per + k + 1] for k in range(per)]
        row = mine[0] if per == 1 else (mine[2] + mine[1]) + mine[0]
        columns.append(to_column(row, traits))
    return wide, columns


def fuse(fn, *args):
    shapes = jax.eval_shape(fn, *args)

    def kernel(*refs):
        ins, outs = refs[: len(args)], refs[len(args) :]
        for out, value in zip(outs, fn(*(ref[...] for ref in ins))):
            out[...] = value

    return pl.pallas_call(kernel, out_shape=shapes, compiler_params=PARAMS, in_specs=[VMEM] * len(args), out_specs=[VMEM] * len(shapes))(*args)


def place_in_quad():
    return lax.axis_index("ppl") & (QUAD - 1)


def prepare(block_index, valid_counts, genotypes, coef_all, noise_coef, residual, noise_people, sigma2_old, prior_prec):
    operands = genotypes, coef_all, noise_coef, valid_counts, residual, noise_people, sigma2_old, prior_prec
    rows, width = genotypes.shape
    traits = residual.shape[0]
    quarter = width // QUAD

    def kernel(block_ref, geno_ref, coef_ref, noise_ref, *refs):
        wanted, x_refs, (noise_out, partial_ref, *refs) = refs[:5], refs[5 : 5 + QUAD], refs[5 + QUAD :]
        kept_ref, given_ref, cross_ref, var_ref, ridge_ref, mask_ref, present_ref, old_ref, *landed, sems = refs
        me = lax.axis_index("ppl")
        own = place_in_quad()
        small = [pltpu.make_async_copy(a, b, sems.at[2 * QUAD + 1 + k]) for k, (a, b) in enumerate(zip(wanted, landed))]
        for copy in small:
            copy.start()
        valid_ref, res_ref, people_ref, sigma_ref, prior_ref = landed
        copies = []
        for slot in range(QUAD):
            span = pl.ds(pl.multiple_of((own ^ slot) * quarter, LANES), quarter)
            first = pl.multiple_of(block_ref[0] * width + (own ^ slot) * quarter, LANES)
            pair = (
                pltpu.make_async_copy(coef_ref.at[:, pl.ds(first, quarter)], old_ref.at[slot], sems.at[QUAD + slot]),
                pltpu.make_async_copy(geno_ref.at[:, span], x_refs[slot], sems.at[slot]),
            )
            for copy in pair:
                copy.start()
            copies.append(pair)
        span = pl.ds(pl.multiple_of(own * quarter, LANES), quarter)
        last = pltpu.make_async_copy(noise_ref.at[:, span], noise_out, sems.at[2 * QUAD])
        last.start()
        for copy in small:
            copy.wait()
        present = sum(valid_ref[k] for k in range(valid_counts.shape[0]))
        present_ref[...] = jnp.full((1, traits), present, jnp.int32).astype(F32)
        noise_var = to_column(sigma_ref[...], traits)
        var_ref[...] = noise_var
        ridge_ref[...] = to_column(prior_ref[...], traits)
        fitted = jnp.zeros((traits, rows), F32)
        for slot in range(QUAD):
            for copy in copies[slot]:
                copy.wait()
            fitted += dot_t(old_ref[slot].astype(BF16), x_refs[slot][...])
        slots = lax.broadcasted_iota(jnp.int32, (1, rows), 1)
        for slot in range(QUAD):
            mask_ref[:, slot * rows : (slot + 1) * rows] = (slots < valid_ref[me ^ slot]).astype(F32)
        present = (slots < valid_ref[me]).astype(F32)
        partial = present * (res_ref[...] + fitted)
        partial_ref[...] = partial
        target = (present * (partial + jnp.sqrt(noise_var) * people_ref[...])).astype(BF16)
        lines = traits * quarter // LANES
        cross_ref[:lines] = pack(dot(target, x_refs[1][...]), (), F32)
        cross_ref[lines:] = pack(dot(target, x_refs[3][...]), (), F32)
        given_ref[...] = pack(dot(target, x_refs[2][...]), (), F32)
        kept_ref[...] = pack(dot(target, x_refs[0][...]), (), F32)
        last.wait()

    lines = traits * quarter // LANES
    shape = jax.ShapeDtypeStruct
    out_shape = [shape((rows, quarter), BF16)] * QUAD + [
        shape((traits, quarter), F32),
        shape((traits, rows), F32),
        shape((lines, LANES), F32),
        shape((lines, LANES), F32),
        shape((2 * lines, LANES), F32),
        shape((traits, 1), F32),
        shape((traits, 1), F32),
        shape((1, QUAD * rows), F32),
        shape((1, traits), F32),
    ]
    return pl.pallas_call(
        kernel,
        compiler_params=PARAMS,
        out_shape=out_shape,
        in_specs=[SMEM] + [HBM] * 8,
        out_specs=[VMEM] * len(out_shape),
        scratch_shapes=[
            pltpu.VMEM((QUAD, traits, quarter), F32),
            pltpu.SMEM(valid_counts.shape, jnp.int32),
            *(pltpu.VMEM(array.shape, F32) for array in (residual, noise_people, sigma2_old, prior_prec)),
            pltpu.SemaphoreType.DMA((2 * QUAD + 6,)),
        ],
    )(block_index, *(pltpu.with_memory_space_constraint(array, pltpu.HBM) for array in operands))


def image_part(search, direction, x):
    low = search.astype(BF16)
    wide = low.astype(F32)
    sums = [row_sum(search * search), row_sum(wide * wide)]
    if direction is not None:
        sums.append(row_sum(wide * direction))
    image = jnp.concatenate([dot_t(low, block) for block in x], axis=1)
    return pack(image, sums, F32), search, low


def halves(kept, back, far):
    total = kept + back[: kept.shape[0]] + far
    high = total.astype(BF16)
    return high, (total - high.astype(F32)).astype(BF16)


def first_search(got0, got1, got2, got3, noise_coef, noise_var, ridge):
    traits, quarter = noise_coef.shape
    total = by_pairs([unpack(got, traits, quarter)[0] for got in (got0, got1, got2, got3)])
    search = total / noise_var + jnp.sqrt(ridge) * noise_coef
    return pack(search, [row_sum(search * search)], BF16), search


def first_image(mask, *rest):
    opened, x = rest[:QUAD], rest[QUAD:]
    rows, quarter = x[0].shape
    lines = (opened[0].shape[0] - TILE) * LANES
    traits = lines // quarter
    opened = [unpack(piece, traits, quarter, 1) for piece in opened]
    norm = by_pairs([columns[0] for _, columns in opened])
    length = by_pairs([row_sum(wide * wide) for wide, _ in opened])
    lows = [wide.astype(BF16) for wide, _ in opened]
    image = mask[:, :rows] * by_pairs([dot_t(low, block) for low, block in zip(lows, x)])
    rounded = image.astype(BF16)
    energy = row_sum(image * rounded.astype(F32))
    parts = [dot(rounded, block) for block in x]
    sent = jnp.concatenate([pack(parts[1], (), F32), pack(parts[3], [energy], F32)], axis=0)
    return pack(parts[0], [energy], F32), pack(parts[2], (), F32), sent, image, norm, length, *lows


def over_core_first(kept, given, back):
    lines = given.shape[0]
    energy = kept[lines:] + back[2 * lines :]
    both = (kept[:lines] + back[:lines], given + back[lines : 2 * lines])
    return tuple(jnp.concatenate([part, energy], axis=0) for part in both)


def over_quad_first(traits, kept, far):
    wide, columns = unpack(kept + far, traits, (kept.shape[0] - TILE) * LANES // traits, 1)
    return (pack(wide, columns, PEOPLE_KIND[0]),)


def next_search(number, got0, got1, got2, got3, search, direction, norm, length, noise_var, ridge, *rest):
    traits, quarter = search.shape
    if number == 1:
        rest_of, x = rest[:QUAD], rest[QUAD:]
        search = search + by_pairs([unpack(got, traits, quarter)[0] for got in rest_of]) / noise_var
    opened = [unpack(got, traits, quarter, 1) for got in (got0, got1, got2, got3)]
    total = by_pairs([wide for wide, _ in opened])
    energy = by_pairs([columns[0] for _, columns in opened])
    step = norm / (energy / noise_var + ridge * length)
    search = search - step * (total / noise_var + ridge * direction)
    fitted = ()
    if number == 2:
        image, image_old, step_old, *x = rest
        fitted = (step_old * image_old + step * image,)
    if number > 2:
        image, fitted, *x = rest
        fitted = (fitted + step * image,)
    return *image_part(search, direction, x), step, *fitted


def cross(packed, way, traits, rows):
    lines = traits * rows // LANES
    blocks = [packed[(slot ^ way) * lines : ((slot ^ way) + 1) * lines] for slot in range(QUAD)]
    return jnp.concatenate(blocks + [packed[QUAD * lines :]], axis=0)


def over_core(kind, count, traits, rows, sent, back):
    total = sent + cross(back, 1, traits, rows)
    if kind == F32:
        return (total,)
    wide, columns = unpack(total, traits, QUAD * rows, count)
    return (pack(wide, columns, kind),)


def new_image(count, sent, back, mask, low, direction, image, norm_old, length):
    traits = low.shape[0]
    rows = mask.shape[1] // QUAD
    wide, columns = unpack(sent, traits, QUAD * rows, count)
    far, far_columns = unpack(cross(back, 2, traits, rows), traits, QUAD * rows, count)
    columns = [a + b for a, b in zip(columns, far_columns)]
    fresh = mask * (wide + far)
    norm, low_low = columns[:2]
    wide = low.astype(F32)
    beta = norm / norm_old
    length = low_low + beta * (2.0 * columns[2] + beta * length)
    return fresh + beta * image, wide + beta * direction, norm, length, beta


def slots_of(wide, rows):
    return [wide[:, slot * rows : (slot + 1) * rows] for slot in range(QUAD)]


def people_part(number, sent, back, mask, low, direction, norm_old, length, *rest):
    kept = ()
    if number == 1:
        image, x = jnp.concatenate(rest[:QUAD], axis=1), rest[QUAD:]
        kept = (image,)
    else:
        image, *x = rest
    state = new_image(3, sent, back, mask, low, direction, image, norm_old, length)
    rounded = state[0].astype(BF16)
    rows = mask.shape[1] // QUAD
    energy = by_pairs([row_sum(part) for part in slots_of(state[0] * rounded.astype(F32), rows)])
    total, at = 0.0, 0
    for block in x:
        total += dot(rounded[:, at : at + block.shape[0]], block)
        at += block.shape[0]
    return pack(total, [energy], PEOPLE_KIND[number]), *state, *kept


def last_sums(sent, back, mask, low, direction, image, norm_old, length, fitted, *partial):
    before = jnp.concatenate(partial, axis=1) - fitted
    image, _, norm, length, beta = new_image(3, sent, back, mask, low, direction, image, norm_old, length)
    rows = mask.shape[1] // QUAD
    products = (image * image.astype(BF16).astype(F32), before * before, before * image, image * image)
    sums = [to_row(by_pairs([row_sum(part) for part in slots_of(product, rows)])) for product in products]
    packed = jnp.concatenate(sums + [jnp.zeros((TILE - len(sums), LANES), F32)], axis=0)
    return packed, before[:, :rows], image[:, :rows], norm, length, beta


def finish(block_index, present, got, norm, length, noise_var, ridge, gamma, before, image, steps, betas, early, late, coef_all):
    traits, quarter = late[0].shape
    rows = image.shape[1]
    width = QUAD * quarter
    blocks = coef_all.shape[1] // width
    kept = ITERS - 1
    args = [*got, norm, length, noise_var, ridge, gamma, before, image, *steps, *betas, *early, *late]
    split = [len(got), 7, kept, kept, kept * QUAD, QUAD]

    def kernel(block_ref, present_ref, *refs):
        groups, at = [], 0
        for size in split:
            groups.append(refs[at : at + size])
            at += size
        coef_ref, out_ref, res_ref, sigma_ref, scratch, sems = refs[at:]
        block, own = block_ref[0], place_in_quad()

        def hold(index):
            span = pl.ds(index * width, width)
            return pltpu.make_async_copy(coef_ref.at[:, span], out_ref.at[:, span], sems.at[index])

        def give(slot):
            start = pl.multiple_of(block * width + (own ^ slot) * quarter, LANES)
            return pltpu.make_async_copy(scratch.at[slot], out_ref.at[:, pl.ds(start, quarter)], sems.at[blocks + slot])

        for index in range(blocks):
            pl.when(block != index)(lambda index=index: hold(index).start())
        got, (norm, length, noise_var, ridge, gamma, before, image), steps, betas, early, late = groups
        total = by_pairs([ref[...] for ref in got]) if len(got) == QUAD else got[0][...]
        energy, squares, mixed, energy_full = (to_column(total[k : k + 1], traits) for k in range(4))
        step = norm[...] / (energy / noise_var[...] + ridge[...] * length[...])
        scale, mix = [], []
        for number in range(ITERS):
            mix = [betas[number - 1][...] * m for m in mix] + [jnp.ones_like(step)]
            now = steps[number][...] if number < kept else step
            scale = [s + now * m for s, m in zip(scale + [jnp.zeros_like(step)], mix)]
        for slot in range(QUAD):
            value = scale[kept] * late[slot][...].astype(F32)
            for k in range(kept):
                value += scale[k] * early[k * QUAD + slot][...].astype(F32)
            scratch[slot] = value
            give(slot).start()
        res_ref[...] = before[...] - step * image[...]
        squares = squares - step * (2.0 * mixed - step * energy_full)
        row = to_row(squares + PRIOR_DOF * PRIOR_SCALE)[:, :traits]
        sigma_ref[...] = row / ((present_ref[...] + PRIOR_DOF) * gamma[...])
        for slot in range(QUAD):
            give(slot).wait()
        for index in range(blocks):
            pl.when(block != index)(lambda index=index: hold(index).wait())

    shape = jax.ShapeDtypeStruct
    return pl.pallas_call(
        kernel,
        compiler_params=PARAMS,
        out_shape=[shape(coef_all.shape, F32), shape((traits, rows), F32), shape((1, traits), F32)],
        in_specs=[SMEM] + [VMEM] * (len(args) + 2),
        out_specs=[HBM, VMEM, VMEM],
        scratch_shapes=[pltpu.VMEM((QUAD, traits, quarter), F32), pltpu.SemaphoreType.DMA((blocks + QUAD,))],
    )(block_index, present, *args, coef_all)


def per_device(
    count,
    genotypes,
    residual,
    noise_people,
    noise_coef,
    coef_all,
    block_index,
    prior_prec,
    sigma2_old,
    gamma_draw,
    valid_counts,
):
    rows, width = genotypes.shape
    traits = residual.shape[0]
    quarter = width // QUAD

    def swap(x, distance):
        return lax.ppermute(x, "ppl", [(i, i ^ distance) for i in range(count)])

    def share(x):
        return [x] + [swap(x, slot) for slot in (1, 2, 3)]

    def over_z(x, columns):
        stride, kind = QUAD, x.dtype
        while True:
            got = [x] + [swap(x, way * stride) for way in (1, 2, 3)]
            stride *= 4
            if stride >= count:
                return got

            def add(*got):
                opened = [unpack(piece, traits, quarter, columns) for piece in got]
                sums = [by_pairs(list(column)) for column in zip(*(c for _, c in opened))]
                return (pack(by_pairs([wide for wide, _ in opened]), sums, kind),)

            if x.shape[0] == TILE:
                x = by_pairs(got)
            else:
                (x,) = fuse(add, *got)

    columns = sigma2_old[None, :], prior_prec[None, :]
    made = prepare(block_index, valid_counts, genotypes, coef_all, noise_coef, residual, noise_people, *columns)
    x_give, made = made[:QUAD], made[QUAD:]
    noise_quarter, partial_res, kept, given, sent, noise_var, ridge, mask, present = made
    lines = kept.shape[0]
    near = swap(x_give[1], 1)
    back = swap(sent, 1)
    given = given + back[lines:]
    far = swap(given, 2)
    first_cut, second_cut = rows * 3 // 4, rows * 3 // 8
    pieces = [swap(x_give[2][:first_cut], 2)]
    high, low_part = fuse(halves, kept, back, far)
    got = over_z(high, 0)
    sent, search = fuse(first_search, *got, noise_quarter, noise_var, ridge)
    spread = share(sent)
    pieces += [swap(x_give[2][first_cut:], 2), swap(x_give[3][:second_cut], 3)]
    rest_of = over_z(low_part, 0)
    kept, given, sent, image, norm, length, *early = fuse(first_image, mask, *spread, *x_give)
    direction = early[0].astype(F32)
    kept, given = fuse(over_core_first, kept, given, swap(sent, 1))
    (sent,) = fuse(functools.partial(over_quad_first, traits), kept, swap(given, 2))
    got = over_z(sent, 1)
    pieces.append(swap(x_give[3][second_cut:], 3))
    pictures = share(image)
    x = [x_give[0], near, *pieces]

    steps, betas = [], []
    for number in range(1, ITERS):
        held = {1: rest_of, 2: (image, *image_old, *steps) if number == 2 else ()}.get(number) or (image, fitted)
        sent, search, low, step, *fitted = fuse(
            functools.partial(next_search, number), *got, search, direction, norm, length, noise_var, ridge, *held, *x
        )
        fitted = fitted[0] if fitted else None
        steps.append(step)
        (sent,) = fuse(functools.partial(over_core, IMAGE_KIND[number], 3, traits, rows), sent, swap(sent, 1))
        back = swap(sent, 2)
        if number == ITERS - 1:
            sent, before, image, norm, length, beta = fuse(
                last_sums, sent, back, mask, low, direction, image, norm, length, fitted, *partial
            )
            betas.append(beta)
            break
        sent, image, direction, norm, length, beta, *image_old = fuse(
            functools.partial(people_part, number), sent, back, mask, low, direction, norm, length, *(pictures if number == 1 else (image,)), *x
        )
        betas.append(beta)
        got = over_z(sent, 1)
        early += share(low)
        if number == 1:
            partial = share(partial_res)

    late = share(low)
    got = over_z(sent, 4)
    coef_new, residual_new, sigma2_new = finish(
        block_index,
        present,
        got,
        norm,
        length,
        noise_var,
        ridge,
        gamma_draw[None, :],
        before,
        image,
        steps,
        betas,
        early,
        late,
        coef_all,
    )
    return (coef_new, residual_new, sigma2_new.reshape(-1))


def solution(mesh):
    return jax.shard_map(
        functools.partial(per_device, mesh.shape["ppl"]),
        mesh=mesh,
        in_specs=(
            P(("trait", "ppl"), None),
            P("trait", "ppl"),
            P("trait", "ppl"),
            P("trait", None),
            P("trait", None),
            P("trait"),
            P("trait"),
            P("trait"),
            P("trait"),
            P("trait"),
        ),
        out_specs=(P("trait", None), P("trait", "ppl"), P("trait")),
        check_vma=False,
    )
```
